32 devices in a mesh: section: 2 (over x), dp: 4 (over z), tensor: 4 (over y, core).
Axes of the slice: x: 2, y: 2, z: 4, core: 2. Of those that a mesh axis runs over, the one named last changes fastest.
Arguments:
- stream: bfloat16 [2, 4, 1024, 1536], P(None, 'dp', 'tensor'), may hold values from -6 to 6
- cotangent: bfloat16 [2, 4, 1024, 1536], P(None, 'dp', 'tensor'), may hold values from -6 to 6
- norm_gain: float32 [2, 1536], P('section'), may hold values from 0.25 to 1.75
- in_zx: bfloat16 [2, 1536, 2, 3072], P('section', 'dp', None, 'tensor'), may hold values from -0.15625 to 0.15625
- in_dt: bfloat16 [2, 1536, 48], P('section', 'dp', 'tensor'), may hold values from -0.15625 to 0.15625
- in_bc: bfloat16 [2, 1536, 256], P('section', 'dp'), may hold values from -0.15625 to 0.15625
- out_proj: bfloat16 [2, 3072, 1536], P('section', 'tensor', 'dp'), may hold values from -0.109375 to 0.109375
- conv_x: float32 [2, 4, 3072], P('section', None, 'tensor'), may hold values from -2 to 2
- conv_x_bias: float32 [2, 3072], P('section', 'tensor'), may hold values from -2 to 2
- conv_bc: float32 [2, 4, 256], P('section'), may hold values from -2 to 2
- conv_bc_bias: float32 [2, 256], P('section'), may hold values from -2 to 2
- dt_bias: float32 [2, 48], P('section', 'tensor'), may hold values from -6 to -2
- a_log: float32 [2, 48], P('section', 'tensor'), may hold values from 0 to 2.8
- d_skip: float32 [2, 48], P('section', 'tensor'), may hold values from 0.5 to 1.5
- gate_gain: float32 [2, 3072], P('section', 'tensor'), may hold values from 0.25 to 1.75
Outputs:
- section_out: bfloat16 [2, 2, 4, 1024, 1536], P('section', None, 'dp', 'tensor')
- input_grad: bfloat16 [2, 2, 4, 1024, 1536], P('section', None, 'dp', 'tensor')
- grad_norm_gain: float32 [2, 1536], P('section')
- grad_in_zx: float32 [2, 1536, 2, 3072], P('section', 'dp', None, 'tensor')
- grad_in_dt: float32 [2, 1536, 48], P('section', 'dp', 'tensor')
- grad_in_bc: float32 [2, 1536, 256], P('section', 'dp')
- grad_out_proj: float32 [2, 3072, 1536], P('section', 'tensor', 'dp')
- grad_conv_x: float32 [2, 4, 3072], P('section', None, 'tensor')
- grad_conv_x_bias: float32 [2, 3072], P('section', 'tensor')
- grad_conv_bc: float32 [2, 4, 256], P('section')
- grad_conv_bc_bias: float32 [2, 256], P('section')
- grad_dt_bias: float32 [2, 48], P('section', 'tensor')
- grad_a_log: float32 [2, 48], P('section', 'tensor')
- grad_d_skip: float32 [2, 48], P('section', 'tensor')
- grad_gate_gain: float32 [2, 3072], P('section', 'tensor')
The draws below stay inside these ranges and needn't reach their ends.
All inputs are finite; a program needn't handle non-finite values.
Results may differ from the reference program's by a relative error of at most 0.014.
Values may be sent and summed in bfloat16 or wider, within the bound.
A program may use at most 320 MiB of HBM per device.

```python
import jax
import jax.numpy as jnp
from jax import lax

D = 1536
H = 48
N = 128
CONV = 4
GROUP = 256
M = 2
L = 1024
DI = 3072
SEQS = 4


def shard_levels(rng, dims, pieces, low, largest):
    loudness, own = 1.0, jax.random.fold_in(rng, 6)
    for position, blocks in pieces:
        draws = jnp.exp(jax.random.uniform(jax.random.fold_in(own, position), (blocks,), jnp.float32, low / len(pieces), largest / len(pieces)))
        loudness = loudness * jnp.repeat(draws, dims[position] // blocks).reshape([-1 if axis == position else 1 for axis in range(len(dims))])
    return loudness


def normal_values(key, dims, scale, bound, shards=(), dtype=jnp.bfloat16):
    entries = scale * jax.random.normal(key, dims, jnp.float32)
    if shards:
        entries = entries * shard_levels(key, dims, shards, -0.22, 0.18)
    return jnp.clip(entries, -bound, bound).astype(dtype)


def setup_inputs(seed: int = 0) -> dict:
    splits = jax.random.split(jax.random.key(seed), 16)
    return {
        "stream": normal_values(splits[0], (M, SEQS, L, D), 1.0, 6.0, ((1, 4), (2, 4))),
        "cotangent": normal_values(splits[1], (M, SEQS, L, D), 1.0, 6.0, ((1, 4), (2, 4))),
        "norm_gain": jnp.clip(1.0 + 0.15 * jax.random.normal(splits[2], (2, D), jnp.float32), 0.25, 1.75),
        "in_zx": normal_values(splits[3], (2, D, 2, DI), D ** -0.5, 0.15625, ((0, 2), (1, 4), (3, 4))),
        "in_dt": normal_values(splits[4], (2, D, H), D ** -0.5, 0.15625, ((0, 2), (1, 4), (2, 4))),
        "in_bc": normal_values(splits[5], (2, D, 2 * N), D ** -0.5, 0.15625, ((0, 2), (1, 4))),
        "out_proj": normal_values(splits[6], (2, DI, D), DI ** -0.5, 0.109375, ((0, 2), (1, 4), (2, 4))),
        "conv_x": normal_values(splits[7], (2, CONV, DI), 0.5, 2.0, ((0, 2), (2, 4)), jnp.float32),
        "conv_x_bias": normal_values(splits[8], (2, DI), 0.5, 2.0, ((0, 2), (1, 4)), jnp.float32),
        "conv_bc": normal_values(splits[9], (2, CONV, 2 * N), 0.5, 2.0, ((0, 2),), jnp.float32),
        "conv_bc_bias": normal_values(splits[10], (2, 2 * N), 0.5, 2.0, ((0, 2),), jnp.float32),
        "dt_bias": jnp.clip(-6.0 + 4.0 * jax.random.uniform(splits[11], (2, H), jnp.float32) ** shard_levels(splits[11], (2, H), ((0, 2), (1, 4)), -0.2, 0.2), -6.0, -2.0),
        "a_log": jnp.clip(2.8 * jax.random.uniform(splits[12], (2, H), jnp.float32) ** shard_levels(splits[12], (2, H), ((0, 2), (1, 4)), -0.2, 0.2), 0.0, 2.8),
        "d_skip": jnp.clip(0.5 + 1.0 * jax.random.uniform(splits[13], (2, H), jnp.float32) ** shard_levels(splits[13], (2, H), ((0, 2), (1, 4)), -0.2, 0.2), 0.5, 1.5),
        "gate_gain": jnp.clip(1.0 + 0.15 * jax.random.normal(splits[14], (2, DI), jnp.float32), 0.25, 1.75),
    }


@jax.custom_vjp
def low(v):
    return lax.optimization_barrier(v.astype(jnp.bfloat16)).astype(jnp.float32)

@jax.custom_vjp
def low_back(v):
    return v

def low_keep(v):
    return (low(v), None)

def low_pass(kept, grad):
    return (grad,)

def back_keep(v):
    return (v, None)

def back_low(kept, grad):
    return (low(grad),)
low.defvjp(low_keep, low_pass)
low_back.defvjp(back_keep, back_low)
EPSILON = 1e-05
PRECISE = lax.Precision.HIGHEST

def matmul(left, right):
    return jnp.dot(left, right, precision=PRECISE, preferred_element_type=jnp.float32)

def causal_conv(signal, kernel, offset):
    length = signal.shape[0]
    padded = jnp.pad(signal, ((CONV - 1, 0), (0, 0)))
    summed = jnp.broadcast_to(offset[None, :], signal.shape)
    for tap_index in range(CONV):
        summed = summed + kernel[tap_index][None, :] * padded[tap_index:tap_index + length]
    return summed

def state_scan(values, dt_values, rates, b_rows, c_rows):
    length, heads_here, head_size = values.shape
    blocks = length // GROUP
    log_decay = jnp.cumsum((dt_values * rates[None, :]).reshape(blocks, GROUP, heads_here), axis=1)
    x_blocks = values.reshape(blocks, GROUP, heads_here, head_size)
    dt_blocks = dt_values.reshape(blocks, GROUP, heads_here)
    b_blocks = b_rows.reshape(blocks, GROUP, -1)
    c_blocks = c_rows.reshape(blocks, GROUP, -1)
    inner_scores = jnp.einsum('ktn,ksn->kts', c_blocks, b_blocks, precision=PRECISE)
    causal = jnp.arange(GROUP)[:, None] >= jnp.arange(GROUP)[None, :]
    decay_gaps = log_decay[:, :, None, :] - log_decay[:, None, :, :]
    mixing = jnp.exp(jnp.where(causal[None, :, :, None], decay_gaps, -1e+30)) * inner_scores[:, :, :, None] * dt_blocks[:, None, :, :]
    within = jnp.einsum('ktsh,kshp->kthp', mixing, x_blocks, precision=PRECISE)
    final_decay = log_decay[:, -1, :]
    to_end = jnp.exp(final_decay[:, None, :] - log_decay) * dt_blocks
    block_states = jnp.einsum('ksh,kshp,ksn->khpn', to_end, x_blocks, b_blocks, precision=PRECISE)

    def advance(running, inputs_now):
        decay_now, fresh_state = inputs_now
        return (decay_now[:, None, None] * running + fresh_state, running)
    _, entering = lax.scan(advance, jnp.zeros(block_states.shape[1:], jnp.float32), (jnp.exp(final_decay), block_states))
    carried = jnp.einsum('ktn,khpn->kthp', c_blocks, entering, precision=PRECISE) * jnp.exp(log_decay)[:, :, :, None]
    return (within + carried).reshape(length, heads_here, head_size)

def mixer(gate_pre, x_pre, bc_pre, dt_pre, conv_x, conv_x_bias, conv_bc, conv_bc_bias, dt_bias, a_log, d_skip):
    x_conv = jax.nn.silu(causal_conv(x_pre, conv_x, conv_x_bias))
    bc_conv = jax.nn.silu(causal_conv(bc_pre, conv_bc, conv_bc_bias))
    dt_values = jax.nn.softplus(dt_pre + dt_bias[None, :])
    heads_here = dt_values.shape[1]
    per_head = x_conv.reshape(x_conv.shape[0], heads_here, -1)
    scanned = state_scan(per_head, dt_values, -jnp.exp(a_log), bc_conv[:, :N], bc_conv[:, N:])
    scanned = scanned + d_skip[None, :, None] * per_head
    return scanned.reshape(x_conv.shape) * jax.nn.silu(gate_pre)

def layer(layer_in, params):
    norm_gain, in_zx, in_dt, in_bc, out_proj, conv_x, conv_x_bias, conv_bc, conv_bc_bias, dt_bias, a_log, d_skip, gate_gain = params
    inv_rms = lax.rsqrt(lax.optimization_barrier(jnp.mean(layer_in * layer_in, axis=-1, keepdims=True)) + EPSILON)
    normed = low(layer_in * inv_rms * norm_gain[None, :])
    gate_pre = low_back(matmul(normed, in_zx[:, 0, :]))
    x_pre = low_back(matmul(normed, in_zx[:, 1, :]))
    dt_pre = low_back(matmul(normed, in_dt))
    bc_pre = low_back(matmul(normed, in_bc))
    gated = mixer(gate_pre, x_pre, bc_pre, dt_pre, conv_x, conv_x_bias, conv_bc, conv_bc_bias, dt_bias, a_log, d_skip)
    gate_scale = lax.rsqrt(lax.optimization_barrier(jnp.mean(gated * gated, axis=-1, keepdims=True)) + EPSILON)
    gate_normed = low(gated * gate_scale * gate_gain[None, :])
    return layer_in + matmul(gate_normed, out_proj)

def reference(stream, cotangent, norm_gain, in_zx, in_dt, in_bc, out_proj, conv_x, conv_x_bias, conv_bc, conv_bc_bias, dt_bias, a_log, d_skip, gate_gain):
    weights = tuple((leaf_value.astype(jnp.float32) for leaf_value in (norm_gain, in_zx, in_dt, in_bc, out_proj, conv_x, conv_x_bias, conv_bc, conv_bc_bias, dt_bias, a_log, d_skip, gate_gain)))
    first_params = tuple((leaf_value[0] for leaf_value in weights))
    second_params = tuple((leaf_value[1] for leaf_value in weights))
    inputs = stream.astype(jnp.float32).reshape(M * SEQS, L, D)
    seeds = cotangent.astype(jnp.float32).reshape(M * SEQS, L, D)

    def run_layer(layer_inputs, params):
        return lax.map(jax.checkpoint(lambda one_seq: layer(one_seq, params)), layer_inputs)
    first_out, first_back = jax.vjp(run_layer, inputs, first_params)
    sent = low(first_out)
    second_out, second_back = jax.vjp(run_layer, sent, second_params)
    sent_grad, second_grads = second_back(seeds)
    sent_low = low(sent_grad)
    first_in_grad, first_grads = first_back(sent_low)
    shape_out = (M, SEQS, L, D)
    section_out = jnp.stack([sent.reshape(shape_out), second_out.reshape(shape_out)]).astype(jnp.bfloat16)
    input_grad = jnp.stack([first_in_grad.reshape(shape_out), sent_low.reshape(shape_out)]).astype(jnp.bfloat16)
    grads = tuple((jnp.stack([first_value, second_value]) for first_value, second_value in zip(first_grads, second_grads)))
    return (section_out, input_grad, grads[0], grads[1], grads[2], grads[3], grads[4], grads[5], grads[6], grads[7], grads[8], grads[9], grads[10], grads[11], grads[12])
```

```python
import functools

import jax
import jax.numpy as jnp
from jax import lax
from jax.sharding import PartitionSpec as P
from jax.experimental import pallas as pl
from jax.experimental.pallas import tpu as pltpu
BF=jnp.bfloat16; F32=jnp.float32
NS=128; Q=128; CONV=4

def dot(a,b): return jnp.dot(a,b,preferred_element_type=F32)
def dot_nt(a,b): return lax.dot_general(a,b,(((1,),(1,)),((),())),preferred_element_type=F32)
def dot_tn(a,b): return lax.dot_general(a,b,(((0,),(0,)),((),())),preferred_element_type=F32)
def dot_hi(a,b): return lax.dot_general(a,b,(((1,),(0,)),((),())),preferred_element_type=F32,precision=lax.Precision.HIGHEST)

def expand(v, spread_ref):
    hi = v.astype(BF)
    lo = (v - hi.astype(F32)).astype(BF)
    return dot(jnp.concatenate([hi, lo], axis=1), spread_ref[...])

def front_chunk(width, pre_ref, par_ref, ext, first):
    taps = [par_ref[k:k+1, :] for k in range(CONV)]
    conv = par_ref[4:5, :] + taps[0]*ext[5:5+Q, :]
    for k in range(1, CONV):
        conv = conv + taps[k]*ext[5+k:5+k+Q, :]
    return conv

def head_rows(pre_ref, par_ref, width):
    raw = pre_ref[:, 2*width+2*NS:] + par_ref[7:8, :NS]
    dt = jnp.maximum(raw, 0.0) + jnp.log1p(jnp.exp(-jnp.abs(raw)))
    rate = -jnp.exp(par_ref[8:9, :NS])
    row = lax.broadcasted_iota(jnp.int32, (Q, Q), 0)
    col = lax.broadcasted_iota(jnp.int32, (Q, Q), 1)
    lower = (row >= col)
    cum = dot_hi(lower.astype(F32), dt*rate)
    return raw, dt, rate, lower, cum

def fwd_kernel(width, pre_ref, par_ref, spread_ref, yn_ref, sq_ref, st_ref, ext, state, ex_dt, ex_e, ex_w):
    step = pl.program_id(0)
    pairs = width//128
    @pl.when(step == 0)
    def _():
        ext[0:8, :] = jnp.zeros((8, ext.shape[1]), F32)
        state[...] = jnp.zeros_like(state)
    ext[8:, :] = pre_ref[:, width:2*width+2*NS]
    conv = front_chunk(width, pre_ref, par_ref, ext, None)
    act = conv*jax.nn.sigmoid(conv)
    ext[0:8, :] = ext[Q:Q+8, :]
    bm = act[:, width:width+NS].astype(BF)
    cm = act[:, width+NS:].astype(BF)
    raw, dt, rate, lower, cum = head_rows(pre_ref, par_ref, width)
    cum_t = cum.T
    ex_dt[...] = expand(dt, spread_ref)
    ex_e[...] = expand(jnp.exp(cum), spread_ref)
    ex_w[...] = expand(jnp.exp(cum[Q-1:Q, :]-cum), spread_ref)
    scores = dot_nt(cm, bm)
    st_ref[0] = state[...].astype(st_ref.dtype)
    bm_t = bm.T
    lane = lax.broadcasted_iota(jnp.int32, (Q, 128), 1)
    squares = jnp.zeros((Q, 128), F32)
    for p in range(pairs):
        sl = slice(128*p, 128*p+128)
        x = act[:, sl]
        xd = x*ex_dt[:, sl]
        st = state[:, sl]
        mixes = []
        for h in (2*p, 2*p+1):
            gap = cum[:, h:h+1]-cum_t[h:h+1, :]
            mixes.append((jnp.exp(jnp.where(lower, gap, -1e30))*scores).astype(BF))
        xdb = xd.astype(BF)
        zero = jnp.zeros_like(xdb)
        both = jnp.concatenate([jnp.where(lane < 64, xdb, zero), jnp.where(lane < 64, zero, xdb)], axis=0)
        y = dot(jnp.concatenate(mixes, axis=1), both)
        y = y + ex_e[:, sl]*dot(cm, st.astype(BF)) + par_ref[6:7, sl]*x
        z = pre_ref[:, sl]
        yg = y*(z*jax.nn.sigmoid(z))
        squares = squares + yg*yg
        yn_ref[:, sl] = (yg*par_ref[5:6, sl]).astype(BF)
        state[:, sl] = ex_e[Q-1:Q, sl]*st + dot(bm_t, (ex_w[:, sl]*xd).astype(BF))
    sq_ref[...] = jnp.sum(squares, axis=1, keepdims=True)

def mixer_fwd(pre, par, spread, width):
    T = pre.shape[0]; n = T//Q
    pw = pre.shape[1]
    return pl.pallas_call(
        functools.partial(fwd_kernel, width),
        grid=(n,),
        in_specs=[pl.BlockSpec((Q, pw), lambda i: (i, 0)),
                  pl.BlockSpec(par.shape, lambda i: (0, 0)),
                  pl.BlockSpec(spread.shape, lambda i: (0, 0))],
        out_specs=[pl.BlockSpec((Q, width), lambda i: (i, 0)),
                   pl.BlockSpec((Q, 1), lambda i: (i, 0)),
                   pl.BlockSpec((1, NS, width), lambda i: (i, 0, 0))],
        out_shape=[jax.ShapeDtypeStruct((T, width), BF), jax.ShapeDtypeStruct((T, 1), F32),
                   jax.ShapeDtypeStruct((n, NS, width), F32)],
        scratch_shapes=[pltpu.VMEM((Q+8, width+2*NS), F32), pltpu.VMEM((NS, width), F32)]
            + [pltpu.VMEM((Q, width), F32)]*3,
        compiler_params=pltpu.CompilerParams(dimension_semantics=("arbitrary",), vmem_limit_bytes=48<<20),
        name="mixer_fwd",
    )(pre, par, spread)

def fold8(v):
    return jnp.sum(v.reshape(v.shape[0]//8, 8, v.shape[1]), axis=0)

def bwd_kernel(width, n_heads, pre_ref, halo_ref, par_ref, spread_ref, gather_ref, st_ref, dh_ref, kap_ref,
               gp_ref, acc_out, ext, dext, dstate, ex_dt, ex_e, ex_w, acc, dact, sums):
    step = pl.program_id(0)
    steps = pl.num_programs(0)
    pairs = width//128
    @pl.when(step == 0)
    def _():
        dext[Q:, :] = jnp.zeros((8, dext.shape[1]), F32)
        dstate[...] = jnp.zeros_like(dstate)
        acc[...] = jnp.zeros_like(acc)
    ext[8:, :] = pre_ref[:, width:2*width+2*NS]
    halo = halo_ref[:, width:2*width+2*NS]
    ext[0:8, :] = jnp.where(step == steps-1, 0.0, halo)
    conv = front_chunk(width, pre_ref, par_ref, ext, None)
    sg = jax.nn.sigmoid(conv)
    act = conv*sg
    bm = act[:, width:width+NS].astype(BF)
    cm = act[:, width+NS:].astype(BF)
    raw, dt, rate, lower, cum = head_rows(pre_ref, par_ref, width)
    cum_t = cum.T
    e_head = jnp.exp(cum)
    ex_dt[...] = expand(dt, spread_ref)
    ex_e[...] = expand(e_head, spread_ref)
    ex_w[...] = expand(jnp.exp(cum[Q-1:Q, :]-cum), spread_ref)
    scores = dot_nt(cm, bm)
    cm_t = cm.T
    lane = lax.broadcasted_iota(jnp.int32, (Q, 128), 1)
    kap = kap_ref[...]
    dscores = jnp.zeros((Q, Q), F32)
    row_sums = jnp.zeros((Q, 128), F32)
    col_rows = []
    dC = jnp.zeros((Q, NS), F32)
    dB = jnp.zeros((Q, NS), F32)
    w_sum = jnp.zeros((Q, 128), F32)
    e_sum = jnp.zeros((Q, 128), F32)
    t_sum = jnp.zeros((Q, 128), F32)
    f_sum = jnp.zeros((8, 128), F32)
    orow = lax.broadcasted_iota(jnp.int32, (2*Q, 128), 0)
    ocol = lax.broadcasted_iota(jnp.int32, (2*Q, 128), 1)
    for p in range(pairs):
        sl = slice(128*p, 128*p+128)
        x = act[:, sl]
        xdt = ex_dt[:, sl]
        xd = x*xdt
        xdb = xd.astype(BF)
        st = st_ref[0, :, sl]
        stb = st.astype(BF)
        zero = jnp.zeros_like(xdb)
        decays, mixes = [], []
        for h in (2*p, 2*p+1):
            gap = cum[:, h:h+1]-cum_t[h:h+1, :]
            decay = jnp.exp(jnp.where(lower, gap, -1e30))
            decays.append(decay)
            mixes.append(decay*scores)
        mixb = [m.astype(BF) for m in mixes]
        both = jnp.concatenate([jnp.where(lane < 64, xdb, zero), jnp.where(lane < 64, zero, xdb)], axis=0)
        y = dot(jnp.concatenate(mixb, axis=1), both)
        e = ex_e[:, sl]
        carried = e*dot(cm, stb)
        y = y + carried + par_ref[6:7, sl]*x
        z = pre_ref[:, sl]
        sz = jax.nn.sigmoid(z)
        silz = z*sz
        yg = y*silz
        dh = dh_ref[:, sl]
        dyg = par_ref[5:6, sl]*dh - yg*kap
        acc[40:48, sl] += fold8(dh*yg)
        dy = dyg*silz
        gp_ref[:, sl] = (dyg*y*(sz+silz*(1.0-sz))).astype(BF)
        acc[48:56, sl] += fold8(dy*x)
        dyb = dy.astype(BF)
        dstack = jnp.concatenate([jnp.where(lane < 64, dyb, zero), jnp.where(lane < 64, zero, dyb)], axis=0)
        dmix = dot_nt(dstack, xdb)
        rbs = []
        for j in range(2):
            dm = dmix[Q*j:Q*j+Q]
            dscores = dscores + decays[j]*dm
            rb = (mixes[j]*dm).astype(BF)
            rbs.append(rb)
            col_rows.append(jnp.sum(rb.astype(F32), axis=0, keepdims=True))
        pick = (ocol == 2*p + (orow >= Q).astype(jnp.int32)).astype(BF)
        row_sums = row_sums + dot(jnp.concatenate(rbs, axis=1), pick)
        dxd = dot_tn(jnp.concatenate(mixb, axis=0), dstack)
        ds = dstate[:, sl]
        dsb = ds.astype(BF)
        w = ex_w[:, sl]
        from_state = w*dot(bm, dsb)
        gat = gather_ref[sl, :]
        w_sum = w_sum + dot((xd*from_state).astype(BF), gat)
        e_sum = e_sum + dot((dy*carried).astype(BF), gat)
        dxd = dxd + from_state
        t_sum = t_sum + dot((x*dxd).astype(BF), gat)
        f_sum = f_sum + dot_hi(ex_e[Q-1:Q, sl]*fold8(st*ds), gat.astype(F32))
        dact[:, sl] = xdt*dxd + par_ref[6:7, sl]*dy
        edy = (e*dy).astype(BF)
        dC = dC + dot_nt(edy, stb)
        dB = dB + dot_nt((w*xd).astype(BF), dsb)
        dstate[:, sl] = ex_e[Q-1:Q, sl]*ds + dot(cm_t, edy)
    dsc = dscores.astype(BF)
    dact[:, width:width+NS] = dB + dot_tn(dsc, cm)
    dact[:, width+NS:] = dC + dot(dsc, bm)
    cols = jnp.concatenate(col_rows + [jnp.zeros((128-len(col_rows), Q), F32)], axis=0).T
    upper = jnp.logical_not(lower) | (lax.broadcasted_iota(jnp.int32, (Q, Q), 0) == lax.broadcasted_iota(jnp.int32, (Q, Q), 1))
    da = dot_hi(upper.astype(F32), row_sums-cols+e_sum) + dot_hi((lower & jnp.logical_not(upper)).astype(F32), w_sum) + jnp.sum(f_sum, axis=0, keepdims=True)
    keep = lane < n_heads
    ddt = da*rate + t_sum
    draw = jnp.where(keep, ddt*jax.nn.sigmoid(raw), 0.0)
    gp_ref[:, 2*width+2*NS:] = draw.astype(BF)
    acc[56:64, 0:128] += fold8(draw)
    acc[56:64, 128:256] += fold8(jnp.where(keep, da*dt*rate, 0.0))
    dconv = dact[...]*(sg+act*(1.0-sg))
    dext[0:Q, :] = dconv
    dpre = par_ref[3:4, :]*dconv
    for k in range(CONV-1):
        dpre = dpre + par_ref[k:k+1, :]*dext[3-k:3-k+Q, :]
    gp_ref[:, width:2*width+2*NS] = dpre.astype(BF)
    for k in range(CONV):
        acc[8*k:8*k+8, :] += fold8(dconv*ext[5+k:5+k+Q, :])
    acc[32:40, :] += fold8(dconv)
    dext[Q:, :] = dext[0:8, :]
    @pl.when(step == steps-1)
    def _():
        rows = [jnp.sum(acc[8*k:8*k+8, :], axis=0, keepdims=True) for k in range(8)]
        acc_out[...] = jnp.concatenate(rows, axis=0)

def mixer_bwd(pre, par, spread, gather, states, dh, kap, width, n_heads):
    T = pre.shape[0]; n = T//Q; pw = pre.shape[1]
    rev = lambda i: n-1-i
    return pl.pallas_call(
        functools.partial(bwd_kernel, width, n_heads),
        grid=(n,),
        in_specs=[pl.BlockSpec((Q, pw), lambda i: (n-1-i, 0)),
                  pl.BlockSpec((8, pw), lambda i: (jnp.maximum((n-1-i)*(Q//8)-1, 0), 0)),
                  pl.BlockSpec(par.shape, lambda i: (0, 0)),
                  pl.BlockSpec(spread.shape, lambda i: (0, 0)),
                  pl.BlockSpec(gather.shape, lambda i: (0, 0)),
                  pl.BlockSpec((1, NS, width), lambda i: (n-1-i, 0, 0)),
                  pl.BlockSpec((Q, width), lambda i: (n-1-i, 0)),
                  pl.BlockSpec((Q, 1), lambda i: (n-1-i, 0))],
        out_specs=[pl.BlockSpec((Q, pw), lambda i: (n-1-i, 0)),
                   pl.BlockSpec((8, width+2*NS), lambda i: (0, 0))],
        out_shape=[jax.ShapeDtypeStruct((T, pw), BF), jax.ShapeDtypeStruct((8, width+2*NS), F32)],
        scratch_shapes=[pltpu.VMEM((Q+8, width+2*NS), F32), pltpu.VMEM((Q+8, width+2*NS), F32), pltpu.VMEM((NS, width), F32)]
            + [pltpu.VMEM((Q, width), F32)]*3
            + [pltpu.VMEM((64, width+2*NS), F32), pltpu.VMEM((Q, width+2*NS), F32), pltpu.VMEM((8, 128), F32)],
        compiler_params=pltpu.CompilerParams(dimension_semantics=("arbitrary",), vmem_limit_bytes=56<<20),
        name="mixer_bwd",
    )(pre, pre, par, spread, gather, states, dh, kap)


EPSILON = 1e-05
HEAD_PAD = 128


def swap_sections(value):
    count = lax.axis_size("section")
    return lax.ppermute(value, "section", [(i, (i + 1) % count) for i in range(count)])


def token_gather(value):
    return lax.all_gather(value, "tensor", axis=0, tiled=True)


def token_scatter(value):
    return lax.psum_scatter(value, "tensor", scatter_dimension=0, tiled=True)


def weight_gather(own, is_first):
    half = own.shape[0] // 2
    low, high = own[:half], own[half:]
    got = swap_sections(jnp.where(is_first, high, low))
    first_piece = jnp.where(is_first, low, got)
    second_piece = jnp.where(is_first, got, high)
    return tuple(
        lax.all_gather(piece, ("dp", "section"), axis=0, tiled=True)
        for piece in (first_piece, second_piece)
    )


def grad_scatter(value):
    return lax.psum_scatter(
        value.astype(BF), ("dp", "section"), scatter_dimension=0, tiled=True
    )


def join_halves(first_part, second_part, is_first):
    own = jnp.where(is_first, first_part, second_part)
    got = swap_sections(jnp.where(is_first, second_part, first_part))
    low = jnp.where(is_first, own, got)
    high = jnp.where(is_first, got, own)
    return jnp.concatenate([low, high], axis=0).astype(F32)


def local(
    stream, cotangent, norm_gain, in_zx, in_dt, in_bc, out_proj, conv_x, conv_x_bias,
    conv_bc, conv_bc_bias, dt_bias, a_log, d_skip, gate_gain,
):
    section = lax.axis_index("section")
    is_first = section == 0
    model = stream.shape[3]
    rows = stream.shape[2]
    width = conv_x.shape[2]
    heads = dt_bias.shape[1]
    shard = in_zx.shape[1]
    total_inner = width * lax.axis_size("tensor")
    wide = width + 2 * NS
    row_start = lax.axis_index("tensor") * rows

    def padded(value):
        return jnp.pad(value, (0, wide - value.shape[0]))[None]

    gain_rows = -(-model // wide)
    own_par = jnp.concatenate(
        [
            jnp.concatenate([conv_x[0], conv_bc[0]], axis=1),
            jnp.concatenate([conv_x_bias[0], conv_bc_bias[0]])[None],
            padded(gate_gain[0]),
            padded(jnp.repeat(d_skip[0], width // heads)),
            padded(dt_bias[0]),
            padded(a_log[0]),
            jnp.pad(norm_gain[0], (0, gain_rows * wide - model)).reshape(gain_rows, wide),
            jnp.zeros((7 - gain_rows, wide), F32),
        ],
        axis=0,
    )
    other_par = swap_sections(own_par)
    pars = (jnp.where(is_first, own_par, other_par), jnp.where(is_first, other_par, own_par))
    gains = tuple(par[9 : 9 + gain_rows].reshape(-1)[:model] for par in pars)

    own_in = jnp.concatenate(
        [
            in_zx[0].reshape(shard, 2 * width),
            in_bc[0],
            jnp.pad(in_dt[0], ((0, 0), (0, HEAD_PAD - heads))),
        ],
        axis=1,
    )
    own_out = out_proj[0].T
    w_in = weight_gather(own_in, is_first)
    w_out = weight_gather(own_out, is_first)

    head_of = jnp.arange(width) // (width // heads)
    spread = (jnp.arange(2 * HEAD_PAD)[:, None] % HEAD_PAD == head_of[None, :]).astype(BF)
    gather = (head_of[:, None] == jnp.arange(HEAD_PAD)[None, :]).astype(BF)

    def forward(layer, u):
        inv = lax.rsqrt(jnp.mean(u * u, axis=1, keepdims=True) + EPSILON)
        xn = token_gather((u * inv * gains[layer][None, :]).astype(BF))
        pre = dot(xn, w_in[layer])
        yn, squares, states = mixer_fwd(pre, pars[layer], spread, width)
        partial = dot_nt(yn, w_out[layer])
        total = token_scatter(partial)
        squares = lax.dynamic_slice_in_dim(lax.psum(squares[:, 0], "tensor"), row_start, rows)
        q = lax.rsqrt(squares / total_inner + EPSILON)[:, None]
        projected = total * q
        return (u + projected).astype(BF), (u, inv, xn, pre, yn, states, q, projected)

    def backward(layer, g, kept):
        u, inv, xn, pre, yn, states, q, projected = kept
        gq = token_gather((g * q).astype(BF))
        kappa = q * q / total_inner * jnp.sum(g * projected, axis=1, keepdims=True)
        kappa = token_gather(kappa)
        dh = dot(gq, w_out[layer])
        gp, acc = mixer_bwd(pre, pars[layer], spread, gather, states, dh, kappa, width, heads)
        dxn = token_scatter(dot_nt(gp, w_in[layer]))
        g_in = dot_tn(xn, gp)
        g_out = dot_tn(gq, yn)
        scaled = dxn * gains[layer][None, :]
        dots = jnp.sum(scaled * u, axis=1, keepdims=True)
        du = g + inv * scaled - u * (inv * inv * inv) * dots / model
        g_gain = jnp.sum(dxn * u * inv, axis=0)
        return du.astype(BF), g_in, g_out, acc, g_gain

    u0 = lax.dynamic_index_in_dim(stream[:, 0], section, 0, False).astype(F32)
    out0, kept0 = forward(0, u0)
    out1, kept1 = forward(1, out0.astype(F32))
    g1 = lax.dynamic_index_in_dim(cotangent[:, 0], section, 0, False).astype(F32)
    du1, g_in1, g_out1, acc1, gain1 = backward(1, g1, kept1)
    half_in1 = grad_scatter(g_in1)
    half_out1 = grad_scatter(g_out1)
    du0, g_in0, g_out0, acc0, gain0 = backward(0, du1.astype(F32), kept0)
    half_in0 = grad_scatter(g_in0)
    half_out0 = grad_scatter(g_out0)
    g_in = join_halves(half_in0, half_in1, is_first)
    g_out = join_halves(half_out0, half_out1, is_first)

    def by_batch(first_value, second_value):
        own = jnp.where(is_first, first_value, second_value)
        got = swap_sections(jnp.where(is_first, second_value, first_value))
        stacked = jnp.stack([jnp.where(is_first, own, got), jnp.where(is_first, got, own)])
        return stacked[None, :, None]

    def minor(acc, gain):
        return jnp.concatenate(
            [acc, jnp.pad(gain, (0, gain_rows * wide - model)).reshape(gain_rows, wide)], axis=0
        )

    both = lax.psum(jnp.stack([minor(acc0, gain0), minor(acc1, gain1)]), ("dp", "section"))
    mine = jnp.where(is_first, both[0], both[1])
    shared_bc, shared_gain, bc_rows = lax.psum(
        (mine[0:5, width:], mine[8:], g_in[:, 2 * width : 2 * width + 2 * NS]), "tensor"
    )
    return (
        by_batch(out0, out1),
        by_batch(du0, du1),
        shared_gain.reshape(-1)[:model][None],
        g_in[:, : 2 * width].reshape(shard, 2, width)[None],
        g_in[:, 2 * width + 2 * NS : 2 * width + 2 * NS + heads][None],
        bc_rows[None],
        g_out.T[None],
        mine[0:4, :width][None],
        mine[4, :width][None],
        shared_bc[0:4][None],
        shared_bc[4][None],
        mine[7, :heads][None],
        mine[7, HEAD_PAD : HEAD_PAD + heads][None],
        mine[6, :width].reshape(heads, -1).sum(axis=1)[None],
        mine[5, :width][None],
    )


def solution(mesh):
    in_specs = (
        P(None, "dp", "tensor", None),
        P(None, "dp", "tensor", None),
        P("section", None),
        P("section", "dp", None, "tensor"),
        P("section", "dp", "tensor"),
        P("section", "dp", None),
        P("section", "tensor", "dp"),
        P("section", None, "tensor"),
        P("section", "tensor"),
        P("section", None, None),
        P("section", None),
        P("section", "tensor"),
        P("section", "tensor"),
        P("section", "tensor"),
        P("section", "tensor"),
    )
    out_specs = (
        P("section", None, "dp", "tensor", None),
        P("section", None, "dp", "tensor", None),
        P("section", None),
        P("section", "dp", None, "tensor"),
        P("section", "dp", "tensor"),
        P("section", "dp", None),
        P("section", "tensor", "dp"),
        P("section", None, "tensor"),
        P("section", "tensor"),
        P("section", None, None),
        P("section", None),
        P("section", "tensor"),
        P("section", "tensor"),
        P("section", "tensor"),
        P("section", "tensor"),
    )
    return jax.shard_map(local, mesh=mesh, in_specs=in_specs, out_specs=out_specs, check_vma=False)
```

```python
import functools

import jax
import jax.numpy as jnp
from jax import lax
from jax.sharding import PartitionSpec as P
from jax.experimental import pallas as pl
from jax.experimental.pallas import tpu as pltpu
BF=jnp.bfloat16; F32=jnp.float32
NS=128; Q=128; CONV=4

def dot(a,b): return jnp.dot(a,b,preferred_element_type=F32)
def dot_nt(a,b): return lax.dot_general(a,b,(((1,),(1,)),((),())),preferred_element_type=F32)
def dot_tn(a,b): return lax.dot_general(a,b,(((0,),(0,)),((),())),preferred_element_type=F32)
def dot_hi(a,b): return lax.dot_general(a,b,(((1,),(0,)),((),())),preferred_element_type=F32,precision=lax.Precision.HIGHEST)

def expand(v, spread_ref):
    hi = v.astype(BF)
    lo = (v - hi.astype(F32)).astype(BF)
    return dot(jnp.concatenate([hi, lo], axis=1), spread_ref[...])

def front_chunk(width, pre_ref, par_ref, ext, first):
    taps = [par_ref[k:k+1, :] for k in range(CONV)]
    conv = par_ref[4:5, :] + taps[0]*ext[5:5+Q, :]
    for k in range(1, CONV):
        conv = conv + taps[k]*ext[5+k:5+k+Q, :]
    return conv

def head_rows(pre_ref, par_ref, width):
    raw = pre_ref[:, 2*width+2*NS:] + par_ref[7:8, :NS]
    dt = jnp.maximum(raw, 0.0) + jnp.log1p(jnp.exp(-jnp.abs(raw)))
    rate = -jnp.exp(par_ref[8:9, :NS])
    row = lax.broadcasted_iota(jnp.int32, (Q, Q), 0)
    col = lax.broadcasted_iota(jnp.int32, (Q, Q), 1)
    lower = (row >= col)
    cum = dot_hi(lower.astype(F32), dt*rate)
    return raw, dt, rate, lower, cum

def fwd_kernel(width, pre_ref, par_ref, spread_ref, yn_ref, sq_ref, st_ref, ext, state, ex_dt, ex_e, ex_w):
    step = pl.program_id(0)
    pairs = width//128
    @pl.when(step == 0)
    def _():
        ext[0:8, :] = jnp.zeros((8, ext.shape[1]), F32)
        state[...] = jnp.zeros_like(state)
    ext[8:, :] = pre_ref[:, width:2*width+2*NS]
    conv = front_chunk(width, pre_ref, par_ref, ext, None)
    act = conv*jax.nn.sigmoid(conv)
    ext[0:8, :] = ext[Q:Q+8, :]
    bm = act[:, width:width+NS].astype(BF)
    cm = act[:, width+NS:].astype(BF)
    raw, dt, rate, lower, cum = head_rows(pre_ref, par_ref, width)
    cum_t = cum.T
    ex_dt[...] = expand(dt, spread_ref)
    ex_e[...] = expand(jnp.exp(cum), spread_ref)
    ex_w[...] = expand(jnp.exp(cum[Q-1:Q, :]-cum), spread_ref)
    scores = dot_nt(cm, bm)
    st_ref[0] = state[...].astype(st_ref.dtype)
    bm_t = bm.T
    lane = lax.broadcasted_iota(jnp.int32, (Q, 128), 1)
    squares = jnp.zeros((Q, 128), F32)
    for p in range(pairs):
        sl = slice(128*p, 128*p+128)
        x = act[:, sl]
        xd = x*ex_dt[:, sl]
        st = state[:, sl]
        mixes = []
        for h in (2*p, 2*p+1):
            gap = cum[:, h:h+1]-cum_t[h:h+1, :]
            mixes.append((jnp.exp(jnp.where(lower, gap, -1e30))*scores).astype(BF))
        xdb = xd.astype(BF)
        zero = jnp.zeros_like(xdb)
        both = jnp.concatenate([jnp.where(lane < 64, xdb, zero), jnp.where(lane < 64, zero, xdb)], axis=0)
        y = dot(jnp.concatenate(mixes, axis=1), both)
        y = y + ex_e[:, sl]*dot(cm, st.astype(BF)) + par_ref[6:7, sl]*x
        z = pre_ref[:, sl]
        yg = y*(z*jax.nn.sigmoid(z))
        squares = squares + yg*yg
        yn_ref[:, sl] = (yg*par_ref[5:6, sl]).astype(BF)
        state[:, sl] = ex_e[Q-1:Q, sl]*st + dot(bm_t, (ex_w[:, sl]*xd).astype(BF))
    sq_ref[...] = lax.dot_general(
        jnp.ones((8, 128), F32), squares, (((1,), (1,)), ((), ())),
        preferred_element_type=F32, precision=lax.Precision.HIGHEST,
    )

def mixer_fwd(pre, par, spread, width):
    T = pre.shape[0]; n = T//Q
    pw = pre.shape[1]
    return pl.pallas_call(
        functools.partial(fwd_kernel, width),
        grid=(n,),
        in_specs=[pl.BlockSpec((Q, pw), lambda i: (i, 0)),
                  pl.BlockSpec(par.shape, lambda i: (0, 0)),
                  pl.BlockSpec(spread.shape, lambda i: (0, 0))],
        out_specs=[pl.BlockSpec((Q, width), lambda i: (i, 0)),
                   pl.BlockSpec((8, Q), lambda i: (i, 0)),
                   pl.BlockSpec((1, NS, width), lambda i: (i, 0, 0))],
        out_shape=[jax.ShapeDtypeStruct((T, width), BF), jax.ShapeDtypeStruct((8*n, Q), F32),
                   jax.ShapeDtypeStruct((n, NS, width), F32)],
        scratch_shapes=[pltpu.VMEM((Q+8, width+2*NS), F32), pltpu.VMEM((NS, width), F32)]
            + [pltpu.VMEM((Q, width), F32)]*3,
        compiler_params=pltpu.CompilerParams(dimension_semantics=("arbitrary",), vmem_limit_bytes=48<<20),
        name="mixer_fwd",
    )(pre, par, spread)

def fold8(v):
    return jnp.sum(v.reshape(v.shape[0]//8, 8, v.shape[1]), axis=0)

def bwd_kernel(width, n_heads, pre_ref, halo_ref, par_ref, spread_ref, gather_ref, st_ref, dh_ref, kap_ref,
               gp_ref, acc_out, ext, dext, dstate, ex_dt, ex_e, ex_w, acc, dact, sums):
    step = pl.program_id(0)
    steps = pl.num_programs(0)
    pairs = width//128
    @pl.when(step == 0)
    def _():
        dext[Q:, :] = jnp.zeros((8, dext.shape[1]), F32)
        dstate[...] = jnp.zeros_like(dstate)
        acc[...] = jnp.zeros_like(acc)
    ext[8:, :] = pre_ref[:, width:2*width+2*NS]
    halo = halo_ref[:, width:2*width+2*NS]
    ext[0:8, :] = jnp.where(step == steps-1, 0.0, halo)
    conv = front_chunk(width, pre_ref, par_ref, ext, None)
    sg = jax.nn.sigmoid(conv)
    act = conv*sg
    bm = act[:, width:width+NS].astype(BF)
    cm = act[:, width+NS:].astype(BF)
    raw, dt, rate, lower, cum = head_rows(pre_ref, par_ref, width)
    cum_t = cum.T
    e_head = jnp.exp(cum)
    ex_dt[...] = expand(dt, spread_ref)
    ex_e[...] = expand(e_head, spread_ref)
    ex_w[...] = expand(jnp.exp(cum[Q-1:Q, :]-cum), spread_ref)
    scores = dot_nt(cm, bm)
    cm_t = cm.T
    lane = lax.broadcasted_iota(jnp.int32, (Q, 128), 1)
    kap = kap_ref[:, 0:1].astype(F32) + kap_ref[:, 1:2].astype(F32)
    dscores = jnp.zeros((Q, Q), F32)
    row_sums = jnp.zeros((Q, 128), F32)
    col_rows = []
    dC = jnp.zeros((Q, NS), F32)
    dB = jnp.zeros((Q, NS), F32)
    w_sum = jnp.zeros((Q, 128), F32)
    e_sum = jnp.zeros((Q, 128), F32)
    t_sum = jnp.zeros((Q, 128), F32)
    f_sum = jnp.zeros((8, 128), F32)
    orow = lax.broadcasted_iota(jnp.int32, (2*Q, 128), 0)
    ocol = lax.broadcasted_iota(jnp.int32, (2*Q, 128), 1)
    for p in range(pairs):
        sl = slice(128*p, 128*p+128)
        x = act[:, sl]
        xdt = ex_dt[:, sl]
        xd = x*xdt
        xdb = xd.astype(BF)
        st = st_ref[0, :, sl]
        stb = st.astype(BF)
        zero = jnp.zeros_like(xdb)
        decays, mixes = [], []
        for h in (2*p, 2*p+1):
            gap = cum[:, h:h+1]-cum_t[h:h+1, :]
            decay = jnp.exp(jnp.where(lower, gap, -1e30))
            decays.append(decay)
            mixes.append(decay*scores)
        mixb = [m.astype(BF) for m in mixes]
        both = jnp.concatenate([jnp.where(lane < 64, xdb, zero), jnp.where(lane < 64, zero, xdb)], axis=0)
        y = dot(jnp.concatenate(mixb, axis=1), both)
        e = ex_e[:, sl]
        carried = e*dot(cm, stb)
        y = y + carried + par_ref[6:7, sl]*x
        z = pre_ref[:, sl]
        sz = jax.nn.sigmoid(z)
        silz = z*sz
        yg = y*silz
        dh = dh_ref[:, sl]
        dyg = par_ref[5:6, sl]*dh - yg*kap
        acc[40:48, sl] += fold8(dh*yg)
        dy = dyg*silz
        gp_ref[:, sl] = (dyg*y*(sz+silz*(1.0-sz))).astype(BF)
        acc[48:56, sl] += fold8(dy*x)
        dyb = dy.astype(BF)
        dstack = jnp.concatenate([jnp.where(lane < 64, dyb, zero), jnp.where(lane < 64, zero, dyb)], axis=0)
        dmix = dot_nt(dstack, xdb)
        rbs = []
        for j in range(2):
            dm = dmix[Q*j:Q*j+Q]
            dscores = dscores + decays[j]*dm
            rb = (mixes[j]*dm).astype(BF)
            rbs.append(rb)
            col_rows.append(jnp.sum(rb.astype(F32), axis=0, keepdims=True))
        pick = (ocol == 2*p + (orow >= Q).astype(jnp.int32)).astype(BF)
        row_sums = row_sums + dot(jnp.concatenate(rbs, axis=1), pick)
        dxd = dot_tn(jnp.concatenate(mixb, axis=0), dstack)
        ds = dstate[:, sl]
        dsb = ds.astype(BF)
        w = ex_w[:, sl]
        from_state = w*dot(bm, dsb)
        gat = gather_ref[sl, :]
        w_sum = w_sum + dot((xd*from_state).astype(BF), gat)
        e_sum = e_sum + dot((dy*carried).astype(BF), gat)
        dxd = dxd + from_state
        t_sum = t_sum + dot((x*dxd).astype(BF), gat)
        f_sum = f_sum + dot_hi(ex_e[Q-1:Q, sl]*fold8(st*ds), gat.astype(F32))
        dact[:, sl] = xdt*dxd + par_ref[6:7, sl]*dy
        edy = (e*dy).astype(BF)
        dC = dC + dot_nt(edy, stb)
        dB = dB + dot_nt((w*xd).astype(BF), dsb)
        dstate[:, sl] = ex_e[Q-1:Q, sl]*ds + dot(cm_t, edy)
    dsc = dscores.astype(BF)
    dact[:, width:width+NS] = dB + dot_tn(dsc, cm)
    dact[:, width+NS:] = dC + dot(dsc, bm)
    cols = jnp.concatenate(col_rows + [jnp.zeros((128-len(col_rows), Q), F32)], axis=0).T
    upper = jnp.logical_not(lower) | (lax.broadcasted_iota(jnp.int32, (Q, Q), 0) == lax.broadcasted_iota(jnp.int32, (Q, Q), 1))
    da = dot_hi(upper.astype(F32), row_sums-cols+e_sum) + dot_hi((lower & jnp.logical_not(upper)).astype(F32), w_sum) + jnp.sum(f_sum, axis=0, keepdims=True)
    keep = lane < n_heads
    ddt = da*rate + t_sum
    draw = jnp.where(keep, ddt*jax.nn.sigmoid(raw), 0.0)
    gp_ref[:, 2*width+2*NS:] = draw.astype(BF)
    acc[56:64, 0:128] += fold8(draw)
    acc[56:64, 128:256] += fold8(jnp.where(keep, da*dt*rate, 0.0))
    dconv = dact[...]*(sg+act*(1.0-sg))
    dext[0:Q, :] = dconv
    dpre = par_ref[3:4, :]*dconv
    for k in range(CONV-1):
        dpre = dpre + par_ref[k:k+1, :]*dext[3-k:3-k+Q, :]
    gp_ref[:, width:2*width+2*NS] = dpre.astype(BF)
    for k in range(CONV):
        acc[8*k:8*k+8, :] += fold8(dconv*ext[5+k:5+k+Q, :])
    acc[32:40, :] += fold8(dconv)
    dext[Q:, :] = dext[0:8, :]
    @pl.when(step == steps-1)
    def _():
        rows = [jnp.sum(acc[8*k:8*k+8, :], axis=0, keepdims=True) for k in range(8)]
        acc_out[...] = jnp.concatenate(rows, axis=0)

def mixer_bwd(pre, par, spread, gather, states, dh, kap, width, n_heads):
    T = pre.shape[0]; n = T//Q; pw = pre.shape[1]
    rev = lambda i: n-1-i
    return pl.pallas_call(
        functools.partial(bwd_kernel, width, n_heads),
        grid=(n,),
        in_specs=[pl.BlockSpec((Q, pw), lambda i: (n-1-i, 0)),
                  pl.BlockSpec((8, pw), lambda i: (jnp.maximum((n-1-i)*(Q//8)-1, 0), 0)),
                  pl.BlockSpec(par.shape, lambda i: (0, 0)),
                  pl.BlockSpec(spread.shape, lambda i: (0, 0)),
                  pl.BlockSpec(gather.shape, lambda i: (0, 0)),
                  pl.BlockSpec((1, NS, width), lambda i: (n-1-i, 0, 0)),
                  pl.BlockSpec((Q, width), lambda i: (n-1-i, 0)),
                  pl.BlockSpec((Q, 128), lambda i: (n-1-i, 0))],
        out_specs=[pl.BlockSpec((Q, pw), lambda i: (n-1-i, 0)),
                   pl.BlockSpec((8, width+2*NS), lambda i: (0, 0))],
        out_shape=[jax.ShapeDtypeStruct((T, pw), BF), jax.ShapeDtypeStruct((8, width+2*NS), F32)],
        scratch_shapes=[pltpu.VMEM((Q+8, width+2*NS), F32), pltpu.VMEM((Q+8, width+2*NS), F32), pltpu.VMEM((NS, width), F32)]
            + [pltpu.VMEM((Q, width), F32)]*3
            + [pltpu.VMEM((64, width+2*NS), F32), pltpu.VMEM((Q, width+2*NS), F32), pltpu.VMEM((8, 128), F32)],
        compiler_params=pltpu.CompilerParams(dimension_semantics=("arbitrary",), vmem_limit_bytes=56<<20),
        name="mixer_bwd",
    )(pre, pre, par, spread, gather, states, dh, kap)


MESH_ID = pl.DeviceIdType.MESH


def peer(axis, index):
    return {axis: index}


def greet(peers):
    barrier = pltpu.get_barrier_semaphore()
    for where in peers:
        pl.semaphore_signal(barrier, inc=1, device_id=where, device_id_type=MESH_ID)
    pl.semaphore_wait(barrier, len(peers))


def remote(src, dst, send_sem, recv_sem, where):
    return pltpu.make_async_remote_copy(
        src_ref=src, dst_ref=dst, send_sem=send_sem, recv_sem=recv_sem,
        device_id=where, device_id_type=MESH_ID,
    )


PIECES = 2


def token_gather_kernel(count, *refs):
    ins, outs = refs[:count], refs[count : 2 * count]
    send_sem, recv_sem, own_sem = refs[2 * count :]
    me = lax.axis_index("tensor")
    near, far = me ^ 1, me ^ 2
    greet((peer("tensor", near), peer("tensor", far)))

    def copies(index):
        source, target = ins[index], outs[index]
        rows = source.shape[0]
        parts = PIECES if index == 0 else 1
        size = rows // parts
        for part in range(parts):
            here = pl.ds(part * size, size)
            own = pl.ds(pl.multiple_of(me * rows + part * size, 16), size)
            other = pl.ds(pl.multiple_of(far * rows + part * size, 16), size)
            to_far = remote(source.at[here], target.at[own], send_sem.at[index, part, 0],
                            recv_sem.at[index, part, 0], peer("tensor", far))
            to_near = remote(source.at[here], target.at[own], send_sem.at[index, part, 1],
                             recv_sem.at[index, part, 1], peer("tensor", near))
            relay = remote(target.at[other], target.at[other], send_sem.at[index, part, 2],
                           recv_sem.at[index, part, 2], peer("tensor", near))
            yield to_far, to_near, relay

    every = [triple for index in range(count) for triple in copies(index)]
    for to_far, _, _ in every:
        to_far.start()
    for _, to_near, _ in every:
        to_near.start()
    locals_ = []
    for index in range(count):
        rows = ins[index].shape[0]
        local_copy = pltpu.make_async_copy(
            ins[index], outs[index].at[pl.ds(pl.multiple_of(me * rows, 16), rows)], own_sem.at[index]
        )
        local_copy.start()
        locals_.append(local_copy)
    for to_far, _, relay in every:
        to_far.wait_recv()
        relay.start()
    for to_far, to_near, relay in every:
        to_near.wait_recv()
        relay.wait_recv()
        to_far.wait_send()
        to_near.wait_send()
        relay.wait_send()
    for local_copy in locals_:
        local_copy.wait()


def token_gather(values, group_id):
    count = len(values)
    n = lax.axis_size("tensor")
    return pl.pallas_call(
        functools.partial(token_gather_kernel, count),
        out_shape=[jax.ShapeDtypeStruct((n * v.shape[0],) + v.shape[1:], v.dtype) for v in values],
        in_specs=[pl.BlockSpec(memory_space=pltpu.VMEM)] * count,
        out_specs=[pl.BlockSpec(memory_space=pl.ANY)] * count,
        scratch_shapes=[
            pltpu.SemaphoreType.DMA((count, PIECES, 3)),
            pltpu.SemaphoreType.DMA((count, PIECES, 3)),
            pltpu.SemaphoreType.DMA((count,)),
        ],
        compiler_params=pltpu.CompilerParams(collective_id=group_id, has_side_effects=True),
        name="token_gather",
    )(*values)


RS_PIECES = 2


def token_scatter_kernel(with_side, *refs):
    if with_side:
        value_ref, side_ref, out_ref, side_out = refs[:4]
        rest = refs[4:]
    else:
        value_ref, out_ref = refs[:2]
        rest = refs[2:]
    from_near, to_far_buf, from_far, send_sem, recv_sem = rest[:5]
    me = lax.axis_index("tensor")
    near, far, cross = me ^ 1, me ^ 2, me ^ 3
    greet((peer("tensor", near), peer("tensor", far)))
    rows = out_ref.shape[0]
    size = rows // RS_PIECES

    def block(index, part):
        return pl.ds(pl.multiple_of(index * rows + part * size, 16), size)

    first, second, third = [], [], []
    for part in range(RS_PIECES):
        here = pl.ds(part * size, size)
        first.append(remote(value_ref.at[block(cross, part)], from_near.at[0, here], send_sem.at[part, 0],
                            recv_sem.at[part, 0], peer("tensor", near)))
        second.append(remote(value_ref.at[block(near, part)], from_near.at[1, here], send_sem.at[part, 1],
                             recv_sem.at[part, 1], peer("tensor", near)))
        third.append(remote(to_far_buf.at[here], from_far.at[here], send_sem.at[part, 2],
                            recv_sem.at[part, 2], peer("tensor", far)))
    for copy in first:
        copy.start()
    if with_side:
        side_near, side_buf, side_far, side_send, side_recv = rest[5:]
        srows = side_out.shape[0]

        def side_block(index):
            return pl.ds(pl.multiple_of(index * srows, 8), srows)

        s1 = remote(side_ref.at[side_block(cross)], side_near.at[0], side_send.at[0], side_recv.at[0], peer("tensor", near))
        s2 = remote(side_ref.at[side_block(near)], side_near.at[1], side_send.at[1], side_recv.at[1], peer("tensor", near))
        s3 = remote(side_buf, side_far, side_send.at[2], side_recv.at[2], peer("tensor", far))
        s1.start()
        s2.start()
    for copy in second:
        copy.start()
    if with_side:
        s1.wait_recv()
        side_buf[...] = side_ref[side_block(far), :] + side_near[0]
        s3.start()
    for part in range(RS_PIECES):
        here = pl.ds(part * size, size)
        first[part].wait_recv()
        to_far_buf[here, :] = (
            value_ref[block(far, part), :].astype(F32) + from_near[0, here, :].astype(F32)
        ).astype(to_far_buf.dtype)
        third[part].start()
    if with_side:
        s2.wait_recv()
        s3.wait_recv()
        side_out[...] = side_ref[side_block(me), :] + side_near[1] + side_far[...]
        s1.wait_send()
        s2.wait_send()
        s3.wait_send()
    for part in range(RS_PIECES):
        here = pl.ds(part * size, size)
        second[part].wait_recv()
        out_ref[here, :] = value_ref[block(me, part), :].astype(F32) + from_near[1, here, :].astype(F32)
    for part in range(RS_PIECES):
        here = pl.ds(part * size, size)
        third[part].wait_recv()
        out_ref[here, :] = out_ref[here, :] + from_far[here, :].astype(F32)
    for copy in first + second + third:
        copy.wait_send()


def token_scatter(value, group_id, side=None):
    n = lax.axis_size("tensor")
    rows, cols = value.shape[0] // n, value.shape[1]
    operands = [value]
    out_shape = [jax.ShapeDtypeStruct((rows, cols), F32)]
    scratch = [
        pltpu.VMEM((2, rows, cols), value.dtype),
        pltpu.VMEM((rows, cols), value.dtype),
        pltpu.VMEM((rows, cols), value.dtype),
        pltpu.SemaphoreType.DMA((RS_PIECES, 3)),
        pltpu.SemaphoreType.DMA((RS_PIECES, 3)),
    ]
    if side is not None:
        srows, scols = side.shape[0] // n, side.shape[1]
        operands.append(side)
        out_shape.append(jax.ShapeDtypeStruct((srows, scols), F32))
        scratch += [
            pltpu.VMEM((2, srows, scols), F32),
            pltpu.VMEM((srows, scols), F32),
            pltpu.VMEM((srows, scols), F32),
            pltpu.SemaphoreType.DMA((3,)),
            pltpu.SemaphoreType.DMA((3,)),
        ]
    return pl.pallas_call(
        functools.partial(token_scatter_kernel, side is not None),
        out_shape=out_shape,
        in_specs=[pl.BlockSpec(memory_space=pltpu.VMEM)] * len(operands),
        out_specs=[pl.BlockSpec(memory_space=pltpu.VMEM)] * len(operands),
        scratch_shapes=scratch,
        compiler_params=pltpu.CompilerParams(collective_id=group_id, has_side_effects=True, vmem_limit_bytes=40 << 20),
        name="token_scatter",
    )(*operands)


def open_kernel(n, pieces, in_ref, out_ref, xn_ref, fin_ref, fout_ref, xall_ref,
                x_ss, x_rs, z_ss, z_rs, own_sem, t_ss, t_rs):
    sec, z, ten = lax.axis_index("section"), lax.axis_index("dp"), lax.axis_index("tensor")
    across = peer("section", 1 - sec)
    near, far = peer("tensor", ten ^ 1), peer("tensor", ten ^ 2)
    barrier = pltpu.get_barrier_semaphore()
    for where in (across, near, far):
        pl.semaphore_signal(barrier, inc=1, device_id=where, device_id_type=MESH_ID)

    @pl.when(z > 0)
    def _():
        pl.semaphore_signal(barrier, inc=1, device_id=peer("dp", z - 1), device_id_type=MESH_ID)

    @pl.when(z < n - 1)
    def _():
        pl.semaphore_signal(barrier, inc=1, device_id=peer("dp", z + 1), device_id_type=MESH_ID)

    pl.semaphore_wait(barrier, 3 + jnp.where(z > 0, 1, 0) + jnp.where(z < n - 1, 1, 0))
    sources, fulls = (in_ref, out_ref), (fin_ref, fout_ref)
    rows = in_ref.shape[0]
    trows = xn_ref.shape[0]

    def place(p, s):
        array, offset, count, _ = pieces[p]
        return fulls[array].at[pl.ds(pl.multiple_of(s * rows + offset, 16), count)]

    def own(p):
        array, offset, count, _ = pieces[p]
        return sources[array].at[pl.ds(offset, count)]

    def to_x(p, s, source):
        return remote(source, place(p, s), x_ss.at[p, s], x_rs.at[p, s], across)

    def to_z(p, s, step, source):
        side = 0 if step > 0 else 1
        return remote(source, place(p, s), z_ss.at[side, p, s], z_rs.at[side, p, s], peer("dp", z + step))

    def got_z(p, s, side):
        remote(own(p), place(p, s), z_ss.at[side, p, 0], z_rs.at[side, p, s], across).wait_recv()

    def spread(p, s, source, right=True, left=True):
        if right:
            @pl.when(z < n - 1)
            def _():
                to_z(p, s, 1, source).start()
        if left:
            @pl.when(z > 0)
            def _():
                to_z(p, s, -1, source).start()

    every = range(len(pieces))
    via = [piece[3] for piece in pieces]
    me = pl.ds(pl.multiple_of(ten * trows, 16), trows)
    other = pl.ds(pl.multiple_of((ten ^ 2) * trows, 16), trows)
    tok_far = remote(xn_ref, xall_ref.at[me], t_ss.at[0], t_rs.at[0], far)
    tok_near = remote(xn_ref, xall_ref.at[me], t_ss.at[1], t_rs.at[1], near)
    tok_relay = remote(xall_ref.at[other], xall_ref.at[other], t_ss.at[2], t_rs.at[2], near)
    tok_own = pltpu.make_async_copy(xn_ref, xall_ref.at[me], own_sem.at[0])
    tok_far.start()
    tok_near.start()
    tok_own.start()

    @pl.when(sec == 0)
    def _():
        for p in every:
            if via[p] == 1:
                to_x(p, z, own(p)).start()
            else:
                spread(p, z, own(p))
        for p in every:
            if via[p] == 0:
                to_x(p, z, own(p)).start()
        for array in (0, 1):
            whole = fulls[array].at[pl.ds(pl.multiple_of(z * rows, 16), rows)]
            pltpu.make_async_copy(sources[array], whole, own_sem.at[1 + array]).start()
        for d in range(1, n):
            for p in every:
                if via[p] == 0:
                    @pl.when(z - d >= 0)
                    def _():
                        got_z(p, z - d, 0)
                        spread(p, z - d, place(p, z - d), left=False)
                        to_x(p, z - d, place(p, z - d)).start()

                    @pl.when(z + d < n)
                    def _():
                        got_z(p, z + d, 1)
                        spread(p, z + d, place(p, z + d), right=False)
                        to_x(p, z + d, place(p, z + d)).start()
        for d in range(1, n):
            s = lax.rem(z + d, n)
            for p in every:
                if via[p] == 1:
                    to_x(p, s, place(p, s)).wait_recv()

    @pl.when(sec == 1)
    def _():
        for p in every:
            if via[p] == 1:
                to_x(p, z, place(p, z)).wait_recv()
                spread(p, z, place(p, z))
        for d in range(1, n):
            for p in every:
                if via[p] == 1:
                    @pl.when(z - d >= 0)
                    def _():
                        got_z(p, z - d, 0)
                        spread(p, z - d, place(p, z - d), left=False)
                        to_x(p, z - d, place(p, z - d)).start()

                    @pl.when(z + d < n)
                    def _():
                        got_z(p, z + d, 1)
                        spread(p, z + d, place(p, z + d), right=False)
                        to_x(p, z + d, place(p, z + d)).start()
        for d in range(n):
            s = lax.rem(z + d, n)
            for p in every:
                if via[p] == 0:
                    to_x(p, s, place(p, s)).wait_recv()

    tok_far.wait_recv()
    tok_relay.start()
    tok_near.wait_recv()
    tok_relay.wait_recv()
    for copy in (tok_far, tok_near, tok_relay):
        copy.wait_send()
    tok_own.wait()

    @pl.when(sec == 0)
    def _():
        for array in (0, 1):
            whole = fulls[array].at[pl.ds(pl.multiple_of(z * rows, 16), rows)]
            pltpu.make_async_copy(sources[array], whole, own_sem.at[1 + array]).wait()

    for p in every:
        for d in range(n):
            s = lax.rem(z + d, n)
            mine = sec == via[p]
            if d == 0:
                sent_x = jnp.logical_or(sec == 0, False)
            else:
                sent_x = mine

            @pl.when(sent_x)
            def _():
                to_x(p, s, place(p, s)).wait_send()

            @pl.when(mine & (s <= z) & (z < n - 1))
            def _():
                to_z(p, s, 1, place(p, s)).wait_send()

            @pl.when(mine & (s >= z) & (z > 0))
            def _():
                to_z(p, s, -1, place(p, s)).wait_send()


def open_gather(own_in, own_out, xn, group_id):
    n = lax.axis_size("dp")
    rows = own_in.shape[0]
    third = rows // 3
    pieces = (
        (0, third, third, 1), (0, 2 * third, third, 1), (0, 0, third, 0),
        (1, third, 2 * third, 1), (1, 0, third, 0),
    )
    count = len(pieces)
    sem = lambda *shape: pltpu.SemaphoreType.DMA(shape)
    return pl.pallas_call(
        functools.partial(open_kernel, n, pieces),
        out_shape=[
            jax.ShapeDtypeStruct((n * rows, own_in.shape[1]), BF),
            jax.ShapeDtypeStruct((n * rows, own_out.shape[1]), BF),
            jax.ShapeDtypeStruct((lax.axis_size("tensor") * xn.shape[0], xn.shape[1]), BF),
        ],
        in_specs=[pl.BlockSpec(memory_space=pltpu.VMEM)] * 3,
        out_specs=[pl.BlockSpec(memory_space=pl.ANY)] * 3,
        scratch_shapes=[sem(count, n), sem(count, n), sem(2, count, n), sem(2, count, n), sem(3), sem(3), sem(3)],
        compiler_params=pltpu.CompilerParams(collective_id=group_id, has_side_effects=True),
        name="weights_open",
    )(own_in, own_out, xn)


CHUNK_ROWS = 16


def by_rows(count, body):
    @pl.loop(0, count // CHUNK_ROWS)
    def _(index):
        body(pl.multiple_of(index * CHUNK_ROWS, CHUNK_ROWS))


def finish_kernel(
    n, shared, g_ref, half_ref, own_ref, send_ref, small_ref,
    gin_ref, gout_ref, small_x_ref, small_t_ref, bc_ref,
    x_recv, z_recv, z_send, last_buf, last_recv, join_recv, out_recv,
    small_recv, small_all, small_ten, bc_own, bc_far, bc_mid, bc_near,
    x_ss, x_rs, z_ss, z_rs, m_ss, m_rs, d_ss, d_rs, t_ss, t_rs,
):
    sec, z, ten = lax.axis_index("section"), lax.axis_index("dp"), lax.axis_index("tensor")
    half = half_ref.shape[0]
    rows = 2 * half
    mine, theirs = sec * half, (1 - sec) * half
    across = peer("section", 1 - sec)
    near, far = peer("tensor", ten ^ 1), peer("tensor", ten ^ 2)
    others = [lax.rem(z + d, n) for d in range(1, n)]
    mates = [ten ^ d for d in range(1, 4)]
    greet([across] + [peer("dp", o) for o in others] + [peer("tensor", t) for t in mates])
    srows = small_recv.shape[0]

    def own_rows(s, offset):
        return pl.ds(pl.multiple_of(s * rows + offset, 16), half)

    small_x = remote(small_ref.at[pl.ds(pl.multiple_of((1 - sec) * srows, 8), srows)], small_recv,
                     m_ss.at[0], m_rs.at[0], across)
    small_x.start()
    order = [i // 2 if i % 2 else n - 1 - i // 2 for i in range(n)]
    x_copies = {}
    for s in order:
        x_copies[s] = remote(g_ref.at[own_rows(s, theirs)], x_recv.at[s], x_ss.at[s], x_rs.at[s], across)
        x_copies[s].start()
    join = remote(half_ref, join_recv, m_ss.at[1], m_rs.at[1], across)
    last = remote(last_buf, last_recv, m_ss.at[2], m_rs.at[2], across)
    out_copy = remote(send_ref, out_recv, m_ss.at[3], m_rs.at[3], across)
    out_copy.start()

    @pl.when(sec == 0)
    def _():
        join.start()

    small_x.wait_recv()
    small_all[z] = small_ref[pl.ds(pl.multiple_of(sec * srows, 8), srows), :] + small_recv[...]
    to_dp = [remote(small_all.at[z], small_all.at[z], d_ss.at[d], d_rs.at[z], peer("dp", o)) for d, o in enumerate(others)]
    for copy in to_dp:
        copy.start()

    def z_copy(s):
        right = s > z
        side = jnp.where(right, 0, 1)
        down = z + jnp.where(right, 1, -1)
        return remote(z_send.at[s], z_recv.at[side, s], z_ss.at[s], z_rs.at[side, s], peer("dp", down))

    def arrived(side, s):
        remote(z_send.at[0], z_recv.at[side, s], z_ss.at[0], z_rs.at[side, s], across).wait_recv()

    for s in order:
        x_copies[s].wait_recv()

        @pl.when(s != z)
        def _():
            right = s > z
            side = jnp.where(right, 0, 1)
            upstream = jnp.where(right, z > 0, z < n - 1)

            @pl.when(upstream)
            def _():
                arrived(side, s)

                def body(r):
                    z_send[s, pl.ds(r, CHUNK_ROWS), :] = (
                        g_ref[pl.ds(pl.multiple_of(s * rows + mine + r, 16), CHUNK_ROWS), :].astype(F32)
                        + x_recv[s, pl.ds(r, CHUNK_ROWS), :].astype(F32)
                        + z_recv[side, s, pl.ds(r, CHUNK_ROWS), :].astype(F32)
                    ).astype(BF)

                by_rows(half, body)

            @pl.when(jnp.logical_not(upstream))
            def _():
                def body(r):
                    z_send[s, pl.ds(r, CHUNK_ROWS), :] = (
                        g_ref[pl.ds(pl.multiple_of(s * rows + mine + r, 16), CHUNK_ROWS), :].astype(F32)
                        + x_recv[s, pl.ds(r, CHUNK_ROWS), :].astype(F32)
                    ).astype(BF)

                by_rows(half, body)

            z_copy(s).start()

    for d, o in enumerate(others):
        remote(small_all.at[o], small_all.at[o], d_ss.at[d], d_rs.at[o], across).wait_recv()
    total = small_all[0]
    for k in range(1, n):
        total = total + small_all[k]
    small_x_ref[...] = total
    small_ten[ten] = total
    to_ten = [remote(small_ten.at[ten], small_ten.at[ten], t_ss.at[d], t_rs.at[ten], peer("tensor", t)) for d, t in enumerate(mates)]
    for copy in to_ten:
        copy.start()

    out_copy.wait_recv()

    def put_out(r):
        gout_ref[pl.ds(pl.multiple_of(mine + r, 16), CHUNK_ROWS), :] = own_ref[pl.ds(r, CHUNK_ROWS), :].astype(F32)
        gout_ref[pl.ds(pl.multiple_of(theirs + r, 16), CHUNK_ROWS), :] = out_recv[pl.ds(r, CHUNK_ROWS), :].astype(F32)

    by_rows(half, put_out)

    def base(r):
        gin_ref[pl.ds(r, CHUNK_ROWS), :] = (
            g_ref[pl.ds(pl.multiple_of(z * rows + mine + r, 16), CHUNK_ROWS), :].astype(F32)
            + x_recv[z, pl.ds(r, CHUNK_ROWS), :].astype(F32)
        )

    by_rows(half, base)
    for side, there in ((0, z > 0), (1, z < n - 1)):

        @pl.when(there)
        def _():
            arrived(side, z)

            def more(r):
                gin_ref[pl.ds(r, CHUNK_ROWS), :] += z_recv[side, z, pl.ds(r, CHUNK_ROWS), :].astype(F32)

            by_rows(half, more)

    @pl.when(sec == 1)
    def _():
        def out(r):
            last_buf[pl.ds(r, CHUNK_ROWS), :] = gin_ref[pl.ds(r, CHUNK_ROWS), :].astype(BF)

        by_rows(half, out)
        last.start()
        join.wait_recv()

        def put(r):
            gin_ref[pl.ds(r, CHUNK_ROWS), :] = join_recv[pl.ds(r, CHUNK_ROWS), :].astype(F32)
            gin_ref[pl.ds(pl.multiple_of(half + r, 16), CHUNK_ROWS), :] = half_ref[pl.ds(r, CHUNK_ROWS), :].astype(F32)

        by_rows(half, put)
        last.wait_send()

    @pl.when(sec == 0)
    def _():
        last.wait_recv()

        def put(r):
            gin_ref[pl.ds(pl.multiple_of(half + r, 16), CHUNK_ROWS), :] = last_recv[pl.ds(r, CHUNK_ROWS), :].astype(F32)

        by_rows(half, put)
        join.wait_send()

    bc_own[...] = gin_ref[:, shared : shared + 2 * NS].astype(BF)
    to_far = remote(bc_own, bc_far, t_ss.at[3], t_rs.at[4], far)
    to_far.start()
    for d, t in enumerate(mates):
        remote(small_ten.at[t], small_ten.at[t], t_ss.at[d], t_rs.at[t], near).wait_recv()
    total = small_ten[0]
    for k in range(1, 4):
        total = total + small_ten[k]
    small_t_ref[...] = total
    to_far.wait_recv()
    bc_mid[...] = (bc_own[...].astype(F32) + bc_far[...].astype(F32)).astype(BF)
    to_near = remote(bc_mid, bc_near, t_ss.at[4], t_rs.at[5], near)
    to_near.start()
    to_near.wait_recv()
    bc_ref[...] = bc_mid[...].astype(F32) + bc_near[...].astype(F32)
    for s in order:
        x_copies[s].wait_send()

        @pl.when(s != z)
        def _():
            z_copy(s).wait_send()

    for copy in [small_x, out_copy, to_far, to_near] + to_dp + to_ten:
        copy.wait_send()


def finish(grads, half_other, out_own, out_send, smalls, shared, group_id):
    n = lax.axis_size("dp")
    half, wide = half_other.shape
    owide = out_own.shape[1]
    srows, swide = smalls.shape[0] // 2, smalls.shape[1]
    vm = lambda shape, dtype: pltpu.VMEM(shape, dtype)
    sem = lambda *shape: pltpu.SemaphoreType.DMA(shape)
    return pl.pallas_call(
        functools.partial(finish_kernel, n, shared),
        out_shape=[
            jax.ShapeDtypeStruct((2 * half, wide), F32),
            jax.ShapeDtypeStruct((2 * half, owide), F32),
            jax.ShapeDtypeStruct((srows, swide), F32),
            jax.ShapeDtypeStruct((srows, swide), F32),
            jax.ShapeDtypeStruct((2 * half, 2 * NS), F32),
        ],
        in_specs=[pl.BlockSpec(memory_space=pltpu.VMEM)] * 5,
        out_specs=[pl.BlockSpec(memory_space=pltpu.VMEM)] * 5,
        scratch_shapes=[
            vm((n, half, wide), BF), vm((2, n, half, wide), BF), vm((n, half, wide), BF),
            vm((half, wide), BF), vm((half, wide), BF), vm((half, wide), BF), vm((half, owide), BF),
            vm((srows, swide), F32), vm((n, srows, swide), F32), vm((4, srows, swide), F32),
            vm((2 * half, 2 * NS), BF), vm((2 * half, 2 * NS), BF), vm((2 * half, 2 * NS), BF), vm((2 * half, 2 * NS), BF),
            sem(n), sem(n), sem(n), sem(2, n), sem(4), sem(4), sem(n), sem(n), sem(5), sem(6),
        ],
        compiler_params=pltpu.CompilerParams(collective_id=group_id, has_side_effects=True, vmem_limit_bytes=60 << 20),
        name="grad_finish",
    )(grads, half_other, out_own, out_send, smalls)


EPSILON = 1e-05
HEAD_PAD = 128
SMALL_ROWS = 16


def swap_sections(value):
    count = lax.axis_size("section")
    return lax.ppermute(value, "section", [(i, (i + 1) % count) for i in range(count)])


def later_gather(own, is_first, after):
    half = own.shape[0] // 2
    low, high = own[:half], own[half:]
    got = lax.ppermute(low, "section", [(1, 0)])
    piece, after = lax.optimization_barrier((jnp.where(is_first, got, high), after))
    return lax.all_gather(piece, ("dp", "section"), axis=0, tiled=True), after


def grad_scatter(value):
    return lax.psum_scatter(value, ("dp", "section"), scatter_dimension=0, tiled=True)


def local(
    stream, cotangent, norm_gain, in_zx, in_dt, in_bc, out_proj, conv_x, conv_x_bias,
    conv_bc, conv_bc_bias, dt_bias, a_log, d_skip, gate_gain,
):
    section = lax.axis_index("section")
    is_first = section == 0
    model = stream.shape[3]
    rows = stream.shape[2]
    width = conv_x.shape[2]
    heads = dt_bias.shape[1]
    shard = in_zx.shape[1]
    total_inner = width * lax.axis_size("tensor")
    wide = width + 2 * NS

    def padded(value):
        return jnp.pad(value, (0, wide - value.shape[0]))[None]

    gain_rows = -(-model // wide)
    own_par = jnp.concatenate(
        [
            jnp.concatenate([conv_x[0], conv_bc[0]], axis=1),
            jnp.concatenate([conv_x_bias[0], conv_bc_bias[0]])[None],
            padded(gate_gain[0]),
            padded(jnp.repeat(d_skip[0], width // heads)),
            padded(dt_bias[0]),
            padded(a_log[0]),
            jnp.pad(norm_gain[0], (0, gain_rows * wide - model)).reshape(gain_rows, wide),
            jnp.zeros((7 - gain_rows, wide), F32),
        ],
        axis=0,
    )
    other_par = swap_sections(own_par)
    pars = (jnp.where(is_first, own_par, other_par), jnp.where(is_first, other_par, own_par))
    gains = tuple(par[9 : 9 + gain_rows].reshape(-1)[:model] for par in pars)

    own_in = jnp.concatenate(
        [
            in_zx[0].reshape(shard, 2 * width),
            in_bc[0],
            jnp.pad(in_dt[0], ((0, 0), (0, HEAD_PAD - heads))),
        ],
        axis=1,
    )
    own_out = out_proj[0].T

    head_of = jnp.arange(width) // (width // heads)
    spread = (jnp.arange(2 * HEAD_PAD)[:, None] % HEAD_PAD == head_of[None, :]).astype(BF)
    gather = (head_of[:, None] == jnp.arange(HEAD_PAD)[None, :]).astype(BF)

    def normed(layer, u):
        inv = lax.rsqrt(jnp.mean(u * u, axis=1, keepdims=True) + EPSILON)
        return inv, (u * inv * gains[layer][None, :]).astype(BF)

    def forward(layer, u, inv, xn, w_in, w_out):
        pre = dot(xn, w_in)
        yn, squares, states = mixer_fwd(pre, pars[layer], spread, width)
        partial = dot_nt(yn, w_out).astype(BF)
        total, squares = token_scatter(partial, 3 + layer, squares)
        q = lax.rsqrt(squares[::8].reshape(rows) / total_inner + EPSILON)[:, None]
        projected = total * q
        return (u + projected).astype(BF), (u, inv, xn, pre, yn, states, q, projected, w_in, w_out)

    def backward(layer, g, kept):
        u, inv, xn, pre, yn, states, q, projected, w_in, w_out = kept
        kappa = q * q / total_inner * jnp.sum(g * projected, axis=1, keepdims=True)
        high = kappa.astype(BF)
        low = (kappa - high.astype(F32)).astype(BF)
        side = jnp.pad(jnp.concatenate([high, low], axis=1), ((0, 0), (0, 126)))
        gq, side = token_gather([(g * q).astype(BF), side], 5 + layer)
        dh = dot(gq, w_out)
        gp, acc = mixer_bwd(pre, pars[layer], spread, gather, states, dh, side, width, heads)
        g_out = dot_tn(gq, yn).astype(BF)
        g_in = dot_tn(xn, gp).astype(BF)
        (dxn,) = token_scatter(dot_nt(gp, w_in).astype(BF), 7 + layer)
        scaled = dxn * gains[layer][None, :]
        dots = jnp.sum(scaled * u, axis=1, keepdims=True)
        du = g + inv * scaled - u * (inv * inv * inv) * dots / model
        g_gain = jnp.sum(dxn * u * inv, axis=0)
        return du.astype(BF), g_in, g_out, acc, g_gain

    u0 = lax.dynamic_index_in_dim(stream[:, 0], section, 0, False).astype(F32)
    inv0, xn0 = normed(0, u0)
    w_in0, w_out0, xn0 = open_gather(own_in, own_out, xn0, 1)
    full_in1, w_in0 = later_gather(own_in, is_first, w_in0)
    full_out1, w_in0 = later_gather(own_out, is_first, w_in0)

    out0, kept0 = forward(0, u0, inv0, xn0, w_in0, w_out0)
    u1 = out0.astype(F32)
    inv1, xn1 = normed(1, u1)
    (xn1,) = token_gather([xn1], 2)
    out1, kept1 = forward(1, u1, inv1, xn1, full_in1, full_out1)
    g1 = lax.dynamic_index_in_dim(cotangent[:, 0], section, 0, False).astype(F32)
    du1, g_in1, g_out1, acc1, gain1 = backward(1, g1, kept1)
    half_out1 = grad_scatter(g_out1)
    half_in1 = grad_scatter(g_in1)
    du0, g_in0, g_out0, acc0, gain0 = backward(0, du1.astype(F32), kept0)
    half_out0 = grad_scatter(g_out0)

    def by_batch(first_value, second_value):
        own = jnp.where(is_first, first_value, second_value)
        got = swap_sections(jnp.where(is_first, second_value, first_value))
        stacked = jnp.stack([jnp.where(is_first, own, got), jnp.where(is_first, got, own)])
        return stacked[None, :, None]

    def minor(acc, gain):
        return jnp.concatenate(
            [
                acc,
                jnp.pad(gain, (0, gain_rows * wide - model)).reshape(gain_rows, wide),
                jnp.zeros((SMALL_ROWS - 8 - gain_rows, wide), F32),
            ],
            axis=0,
        )

    smalls = jnp.concatenate([minor(acc0, gain0), minor(acc1, gain1)])
    g_in, g_out, mine, shared, bc_rows = finish(
        g_in0, half_in1, jnp.where(is_first, half_out0, half_out1),
        jnp.where(is_first, half_out1, half_out0), smalls, 2 * width, 9,
    )
    return (
        by_batch(out0, out1),
        by_batch(du0, du1),
        shared[8 : 8 + gain_rows].reshape(-1)[:model][None],
        g_in[:, : 2 * width].reshape(shard, 2, width)[None],
        g_in[:, 2 * width + 2 * NS : 2 * width + 2 * NS + heads][None],
        bc_rows[None],
        g_out.T[None],
        mine[0:4, :width][None],
        mine[4, :width][None],
        shared[0:4, width:][None],
        shared[4, width:][None],
        mine[7, :heads][None],
        mine[7, HEAD_PAD : HEAD_PAD + heads][None],
        mine[6, :width].reshape(heads, -1).sum(axis=1)[None],
        mine[5, :width][None],
    )


def solution(mesh):
    in_specs = (
        P(None, "dp", "tensor", None),
        P(None, "dp", "tensor", None),
        P("section", None),
        P("section", "dp", None, "tensor"),
        P("section", "dp", "tensor"),
        P("section", "dp", None),
        P("section", "tensor", "dp"),
        P("section", None, "tensor"),
        P("section", "tensor"),
        P("section", None, None),
        P("section", None),
        P("section", "tensor"),
        P("section", "tensor"),
        P("section", "tensor"),
        P("section", "tensor"),
    )
    out_specs = (
        P("section", None, "dp", "tensor", None),
        P("section", None, "dp", "tensor", None),
        P("section", None),
        P("section", "dp", None, "tensor"),
        P("section", "dp", "tensor"),
        P("section", "dp", None),
        P("section", "tensor", "dp"),
        P("section", None, "tensor"),
        P("section", "tensor"),
        P("section", None, None),
        P("section", None),
        P("section", "tensor"),
        P("section", "tensor"),
        P("section", "tensor"),
        P("section", "tensor"),
    )
    return jax.shard_map(local, mesh=mesh, in_specs=in_specs, out_specs=out_specs, check_vma=False)
```

```python
import functools

import jax
import jax.numpy as jnp
from jax import lax
from jax.sharding import PartitionSpec as P
from jax.experimental import pallas as pl
from jax.experimental.pallas import tpu as pltpu
BF=jnp.bfloat16; F32=jnp.float32
NS=128; Q=128; CONV=4


def cost(us):
    return pl.CostEstimate(flops=us * 700_000_000, bytes_accessed=us * 1_500_000, transcendentals=0)


def dot(a,b): return jnp.dot(a,b,preferred_element_type=F32)
def dot_nt(a,b): return lax.dot_general(a,b,(((1,),(1,)),((),())),preferred_element_type=F32)
def dot_tn(a,b): return lax.dot_general(a,b,(((0,),(0,)),((),())),preferred_element_type=F32)
def dot_hi(a,b): return lax.dot_general(a,b,(((1,),(0,)),((),())),preferred_element_type=F32,precision=lax.Precision.HIGHEST)

def expand(v, spread_ref):
    hi = v.astype(BF)
    lo = (v - hi.astype(F32)).astype(BF)
    return dot(jnp.concatenate([hi, lo], axis=1), spread_ref[...])

def front_chunk(width, pre_ref, par_ref, ext, first):
    taps = [par_ref[k:k+1, :] for k in range(CONV)]
    conv = par_ref[4:5, :] + taps[0]*ext[5:5+Q, :]
    for k in range(1, CONV):
        conv = conv + taps[k]*ext[5+k:5+k+Q, :]
    return conv

def head_rows(pre_ref, par_ref, width):
    raw = pre_ref[:, 2*width+2*NS:] + par_ref[7:8, :NS]
    dt = jnp.maximum(raw, 0.0) + jnp.log1p(jnp.exp(-jnp.abs(raw)))
    rate = -jnp.exp(par_ref[8:9, :NS])
    row = lax.broadcasted_iota(jnp.int32, (Q, Q), 0)
    col = lax.broadcasted_iota(jnp.int32, (Q, Q), 1)
    lower = (row >= col)
    cum = dot_hi(lower.astype(F32), dt*rate)
    return raw, dt, rate, lower, cum

def fwd_kernel(width, pre_ref, par_ref, spread_ref, yn_ref, sq_ref, st_ref, ext, state, ex_dt, ex_e, ex_w):
    step = pl.program_id(0)
    pairs = width//128
    @pl.when(step == 0)
    def _():
        ext[0:8, :] = jnp.zeros((8, ext.shape[1]), F32)
        state[...] = jnp.zeros_like(state)
    ext[8:, :] = pre_ref[:, width:2*width+2*NS]
    conv = front_chunk(width, pre_ref, par_ref, ext, None)
    act = conv*jax.nn.sigmoid(conv)
    ext[0:8, :] = ext[Q:Q+8, :]
    bm = act[:, width:width+NS].astype(BF)
    cm = act[:, width+NS:].astype(BF)
    raw, dt, rate, lower, cum = head_rows(pre_ref, par_ref, width)
    cum_t = cum.T
    ex_dt[...] = expand(dt, spread_ref)
    ex_e[...] = expand(jnp.exp(cum), spread_ref)
    ex_w[...] = expand(jnp.exp(cum[Q-1:Q, :]-cum), spread_ref)
    scores = dot_nt(cm, bm)
    st_ref[0] = state[...].astype(st_ref.dtype)
    bm_t = bm.T
    lane = lax.broadcasted_iota(jnp.int32, (Q, 128), 1)
    squares = jnp.zeros((Q, 128), F32)
    for p in range(pairs):
        sl = slice(128*p, 128*p+128)
        x = act[:, sl]
        xd = x*ex_dt[:, sl]
        st = state[:, sl]
        mixes = []
        for h in (2*p, 2*p+1):
            gap = cum[:, h:h+1]-cum_t[h:h+1, :]
            mixes.append((jnp.exp(jnp.where(lower, gap, -1e30))*scores).astype(BF))
        xdb = xd.astype(BF)
        zero = jnp.zeros_like(xdb)
        both = jnp.concatenate([jnp.where(lane < 64, xdb, zero), jnp.where(lane < 64, zero, xdb)], axis=0)
        y = dot(jnp.concatenate(mixes, axis=1), both)
        y = y + ex_e[:, sl]*dot(cm, st.astype(BF)) + par_ref[6:7, sl]*x
        z = pre_ref[:, sl]
        yg = y*(z*jax.nn.sigmoid(z))
        squares = squares + yg*yg
        yn_ref[:, sl] = (yg*par_ref[5:6, sl]).astype(BF)
        state[:, sl] = ex_e[Q-1:Q, sl]*st + dot(bm_t, (ex_w[:, sl]*xd).astype(BF))
    sq_ref[...] = lax.dot_general(
        jnp.ones((8, 128), F32), squares, (((1,), (1,)), ((), ())),
        preferred_element_type=F32, precision=lax.Precision.HIGHEST,
    )

def mixer_fwd(pre, par, spread, width):
    T = pre.shape[0]; n = T//Q
    pw = pre.shape[1]
    return pl.pallas_call(
        functools.partial(fwd_kernel, width),
        grid=(n,),
        in_specs=[pl.BlockSpec((Q, pw), lambda i: (i, 0)),
                  pl.BlockSpec(par.shape, lambda i: (0, 0)),
                  pl.BlockSpec(spread.shape, lambda i: (0, 0))],
        out_specs=[pl.BlockSpec((Q, width), lambda i: (i, 0)),
                   pl.BlockSpec((8, Q), lambda i: (i, 0)),
                   pl.BlockSpec((1, NS, width), lambda i: (i, 0, 0))],
        out_shape=[jax.ShapeDtypeStruct((T, width), BF), jax.ShapeDtypeStruct((8*n, Q), F32),
                   jax.ShapeDtypeStruct((n, NS, width), F32)],
        scratch_shapes=[pltpu.VMEM((Q+8, width+2*NS), F32), pltpu.VMEM((NS, width), F32)]
            + [pltpu.VMEM((Q, width), F32)]*3,
        compiler_params=pltpu.CompilerParams(dimension_semantics=("arbitrary",), vmem_limit_bytes=48<<20),
        cost_estimate=cost(12),
        name="mixer_fwd",
    )(pre, par, spread)

def fold8(v):
    return jnp.sum(v.reshape(v.shape[0]//8, 8, v.shape[1]), axis=0)

def bwd_kernel(width, n_heads, pre_ref, halo_ref, par_ref, spread_ref, gather_ref, st_ref, dh_ref, kap_ref,
               gp_ref, acc_out, ext, dext, dstate, ex_dt, ex_e, ex_w, acc, dact, sums):
    step = pl.program_id(0)
    steps = pl.num_programs(0)
    pairs = width//128
    @pl.when(step == 0)
    def _():
        dext[Q:, :] = jnp.zeros((8, dext.shape[1]), F32)
        dstate[...] = jnp.zeros_like(dstate)
        acc[...] = jnp.zeros_like(acc)
    ext[8:, :] = pre_ref[:, width:2*width+2*NS]
    halo = halo_ref[:, width:2*width+2*NS]
    ext[0:8, :] = jnp.where(step == steps-1, 0.0, halo)
    conv = front_chunk(width, pre_ref, par_ref, ext, None)
    sg = jax.nn.sigmoid(conv)
    act = conv*sg
    bm = act[:, width:width+NS].astype(BF)
    cm = act[:, width+NS:].astype(BF)
    raw, dt, rate, lower, cum = head_rows(pre_ref, par_ref, width)
    cum_t = cum.T
    e_head = jnp.exp(cum)
    ex_dt[...] = expand(dt, spread_ref)
    ex_e[...] = expand(e_head, spread_ref)
    ex_w[...] = expand(jnp.exp(cum[Q-1:Q, :]-cum), spread_ref)
    scores = dot_nt(cm, bm)
    cm_t = cm.T
    lane = lax.broadcasted_iota(jnp.int32, (Q, 128), 1)
    kap = kap_ref[:, 0:1].astype(F32) + kap_ref[:, 1:2].astype(F32)
    dscores = jnp.zeros((Q, Q), F32)
    row_sums = jnp.zeros((Q, 128), F32)
    col_rows = []
    dC = jnp.zeros((Q, NS), F32)
    dB = jnp.zeros((Q, NS), F32)
    w_sum = jnp.zeros((Q, 128), F32)
    e_sum = jnp.zeros((Q, 128), F32)
    t_sum = jnp.zeros((Q, 128), F32)
    f_sum = jnp.zeros((8, 128), F32)
    orow = lax.broadcasted_iota(jnp.int32, (2*Q, 128), 0)
    ocol = lax.broadcasted_iota(jnp.int32, (2*Q, 128), 1)
    for p in range(pairs):
        sl = slice(128*p, 128*p+128)
        x = act[:, sl]
        xdt = ex_dt[:, sl]
        xd = x*xdt
        xdb = xd.astype(BF)
        st = st_ref[0, :, sl]
        stb = st.astype(BF)
        zero = jnp.zeros_like(xdb)
        decays, mixes = [], []
        for h in (2*p, 2*p+1):
            gap = cum[:, h:h+1]-cum_t[h:h+1, :]
            decay = jnp.exp(jnp.where(lower, gap, -1e30))
            decays.append(decay)
            mixes.append(decay*scores)
        mixb = [m.astype(BF) for m in mixes]
        both = jnp.concatenate([jnp.where(lane < 64, xdb, zero), jnp.where(lane < 64, zero, xdb)], axis=0)
        y = dot(jnp.concatenate(mixb, axis=1), both)
        e = ex_e[:, sl]
        carried = e*dot(cm, stb)
        y = y + carried + par_ref[6:7, sl]*x
        z = pre_ref[:, sl]
        sz = jax.nn.sigmoid(z)
        silz = z*sz
        yg = y*silz
        dh = dh_ref[:, sl]
        dyg = par_ref[5:6, sl]*dh - yg*kap
        acc[40:48, sl] += fold8(dh*yg)
        dy = dyg*silz
        gp_ref[:, sl] = (dyg*y*(sz+silz*(1.0-sz))).astype(BF)
        acc[48:56, sl] += fold8(dy*x)
        dyb = dy.astype(BF)
        dstack = jnp.concatenate([jnp.where(lane < 64, dyb, zero), jnp.where(lane < 64, zero, dyb)], axis=0)
        dmix = dot_nt(dstack, xdb)
        rbs = []
        for j in range(2):
            dm = dmix[Q*j:Q*j+Q]
            dscores = dscores + decays[j]*dm
            rb = (mixes[j]*dm).astype(BF)
            rbs.append(rb)
            col_rows.append(jnp.sum(rb.astype(F32), axis=0, keepdims=True))
        pick = (ocol == 2*p + (orow >= Q).astype(jnp.int32)).astype(BF)
        row_sums = row_sums + dot(jnp.concatenate(rbs, axis=1), pick)
        dxd = dot_tn(jnp.concatenate(mixb, axis=0), dstack)
        ds = dstate[:, sl]
        dsb = ds.astype(BF)
        w = ex_w[:, sl]
        from_state = w*dot(bm, dsb)
        gat = gather_ref[sl, :]
        w_sum = w_sum + dot((xd*from_state).astype(BF), gat)
        e_sum = e_sum + dot((dy*carried).astype(BF), gat)
        dxd = dxd + from_state
        t_sum = t_sum + dot((x*dxd).astype(BF), gat)
        f_sum = f_sum + dot_hi(ex_e[Q-1:Q, sl]*fold8(st*ds), gat.astype(F32))
        dact[:, sl] = xdt*dxd + par_ref[6:7, sl]*dy
        edy = (e*dy).astype(BF)
        dC = dC + dot_nt(edy, stb)
        dB = dB + dot_nt((w*xd).astype(BF), dsb)
        dstate[:, sl] = ex_e[Q-1:Q, sl]*ds + dot(cm_t, edy)
    dsc = dscores.astype(BF)
    dact[:, width:width+NS] = dB + dot_tn(dsc, cm)
    dact[:, width+NS:] = dC + dot(dsc, bm)
    cols = jnp.concatenate(col_rows + [jnp.zeros((128-len(col_rows), Q), F32)], axis=0).T
    upper = jnp.logical_not(lower) | (lax.broadcasted_iota(jnp.int32, (Q, Q), 0) == lax.broadcasted_iota(jnp.int32, (Q, Q), 1))
    da = dot_hi(upper.astype(F32), row_sums-cols+e_sum) + dot_hi((lower & jnp.logical_not(upper)).astype(F32), w_sum) + jnp.sum(f_sum, axis=0, keepdims=True)
    keep = lane < n_heads
    ddt = da*rate + t_sum
    draw = jnp.where(keep, ddt*jax.nn.sigmoid(raw), 0.0)
    gp_ref[:, 2*width+2*NS:] = draw.astype(BF)
    acc[56:64, 0:128] += fold8(draw)
    acc[56:64, 128:256] += fold8(jnp.where(keep, da*dt*rate, 0.0))
    dconv = dact[...]*(sg+act*(1.0-sg))
    dext[0:Q, :] = dconv
    dpre = par_ref[3:4, :]*dconv
    for k in range(CONV-1):
        dpre = dpre + par_ref[k:k+1, :]*dext[3-k:3-k+Q, :]
    gp_ref[:, width:2*width+2*NS] = dpre.astype(BF)
    for k in range(CONV):
        acc[8*k:8*k+8, :] += fold8(dconv*ext[5+k:5+k+Q, :])
    acc[32:40, :] += fold8(dconv)
    dext[Q:, :] = dext[0:8, :]
    @pl.when(step == steps-1)
    def _():
        rows = [jnp.sum(acc[8*k:8*k+8, :], axis=0, keepdims=True) for k in range(8)]
        acc_out[...] = jnp.concatenate(rows, axis=0)

def mixer_bwd(pre, par, spread, gather, states, dh, kap, width, n_heads):
    T = pre.shape[0]; n = T//Q; pw = pre.shape[1]
    rev = lambda i: n-1-i
    return pl.pallas_call(
        functools.partial(bwd_kernel, width, n_heads),
        grid=(n,),
        in_specs=[pl.BlockSpec((Q, pw), lambda i: (n-1-i, 0)),
                  pl.BlockSpec((8, pw), lambda i: (jnp.maximum((n-1-i)*(Q//8)-1, 0), 0)),
                  pl.BlockSpec(par.shape, lambda i: (0, 0)),
                  pl.BlockSpec(spread.shape, lambda i: (0, 0)),
                  pl.BlockSpec(gather.shape, lambda i: (0, 0)),
                  pl.BlockSpec((1, NS, width), lambda i: (n-1-i, 0, 0)),
                  pl.BlockSpec((Q, width), lambda i: (n-1-i, 0)),
                  pl.BlockSpec((Q, 128), lambda i: (n-1-i, 0))],
        out_specs=[pl.BlockSpec((Q, pw), lambda i: (n-1-i, 0)),
                   pl.BlockSpec((8, width+2*NS), lambda i: (0, 0))],
        out_shape=[jax.ShapeDtypeStruct((T, pw), BF), jax.ShapeDtypeStruct((8, width+2*NS), F32)],
        scratch_shapes=[pltpu.VMEM((Q+8, width+2*NS), F32), pltpu.VMEM((Q+8, width+2*NS), F32), pltpu.VMEM((NS, width), F32)]
            + [pltpu.VMEM((Q, width), F32)]*3
            + [pltpu.VMEM((64, width+2*NS), F32), pltpu.VMEM((Q, width+2*NS), F32), pltpu.VMEM((8, 128), F32)],
        compiler_params=pltpu.CompilerParams(dimension_semantics=("arbitrary",), vmem_limit_bytes=56<<20),
        cost_estimate=cost(40),
        name="mixer_bwd",
    )(pre, pre, par, spread, gather, states, dh, kap)


MESH_ID = pl.DeviceIdType.MESH


def peer(axis, index):
    return {axis: index}


def greet(peers):
    barrier = pltpu.get_barrier_semaphore()
    for where in peers:
        pl.semaphore_signal(barrier, inc=1, device_id=where, device_id_type=MESH_ID)
    pl.semaphore_wait(barrier, len(peers))


def remote(src, dst, send_sem, recv_sem, where):
    return pltpu.make_async_remote_copy(
        src_ref=src, dst_ref=dst, send_sem=send_sem, recv_sem=recv_sem,
        device_id=where, device_id_type=MESH_ID,
    )


PIECES = 2


def token_gather_kernel(count, *refs):
    ins, outs = refs[:count], refs[count : 2 * count]
    send_sem, recv_sem, own_sem = refs[2 * count :]
    me = lax.axis_index("tensor")
    near, far = me ^ 1, me ^ 2
    greet((peer("tensor", near), peer("tensor", far)))

    def copies(index):
        source, target = ins[index], outs[index]
        rows = source.shape[0]
        parts = PIECES if index == 0 else 1
        size = rows // parts
        for part in range(parts):
            here = pl.ds(part * size, size)
            own = pl.ds(pl.multiple_of(me * rows + part * size, 16), size)
            other = pl.ds(pl.multiple_of(far * rows + part * size, 16), size)
            to_far = remote(source.at[here], target.at[own], send_sem.at[index, part, 0],
                            recv_sem.at[index, part, 0], peer("tensor", far))
            to_near = remote(source.at[here], target.at[own], send_sem.at[index, part, 1],
                             recv_sem.at[index, part, 1], peer("tensor", near))
            relay = remote(target.at[other], target.at[other], send_sem.at[index, part, 2],
                           recv_sem.at[index, part, 2], peer("tensor", near))
            yield to_far, to_near, relay

    every = [triple for index in range(count) for triple in copies(index)]
    for to_far, _, _ in every:
        to_far.start()
    for _, to_near, _ in every:
        to_near.start()
    locals_ = []
    for index in range(count):
        rows = ins[index].shape[0]
        local_copy = pltpu.make_async_copy(
            ins[index], outs[index].at[pl.ds(pl.multiple_of(me * rows, 16), rows)], own_sem.at[index]
        )
        local_copy.start()
        locals_.append(local_copy)
    for to_far, _, relay in every:
        to_far.wait_recv()
        relay.start()
    for to_far, to_near, relay in every:
        to_near.wait_recv()
        relay.wait_recv()
        to_far.wait_send()
        to_near.wait_send()
        relay.wait_send()
    for local_copy in locals_:
        local_copy.wait()


def token_gather(values, group_id):
    count = len(values)
    n = lax.axis_size("tensor")
    return pl.pallas_call(
        functools.partial(token_gather_kernel, count),
        out_shape=[jax.ShapeDtypeStruct((n * v.shape[0],) + v.shape[1:], v.dtype) for v in values],
        in_specs=[pl.BlockSpec(memory_space=pltpu.VMEM)] * count,
        out_specs=[pl.BlockSpec(memory_space=pl.ANY)] * count,
        scratch_shapes=[
            pltpu.SemaphoreType.DMA((count, PIECES, 3)),
            pltpu.SemaphoreType.DMA((count, PIECES, 3)),
            pltpu.SemaphoreType.DMA((count,)),
        ],
        cost_estimate=cost(22),
        compiler_params=pltpu.CompilerParams(collective_id=group_id, has_side_effects=True),
        name="token_gather",
    )(*values)


RS_PIECES = 2


def token_scatter_kernel(with_side, *refs):
    if with_side:
        value_ref, side_ref, out_ref, side_out = refs[:4]
        rest = refs[4:]
    else:
        value_ref, out_ref = refs[:2]
        rest = refs[2:]
    from_near, to_far_buf, from_far, send_sem, recv_sem = rest[:5]
    me = lax.axis_index("tensor")
    near, far, cross = me ^ 1, me ^ 2, me ^ 3
    greet((peer("tensor", near), peer("tensor", far)))
    rows = out_ref.shape[0]
    size = rows // RS_PIECES

    def block(index, part):
        return pl.ds(pl.multiple_of(index * rows + part * size, 16), size)

    first, second, third = [], [], []
    for part in range(RS_PIECES):
        here = pl.ds(part * size, size)
        first.append(remote(value_ref.at[block(cross, part)], from_near.at[0, here], send_sem.at[part, 0],
                            recv_sem.at[part, 0], peer("tensor", near)))
        second.append(remote(value_ref.at[block(near, part)], from_near.at[1, here], send_sem.at[part, 1],
                             recv_sem.at[part, 1], peer("tensor", near)))
        third.append(remote(to_far_buf.at[here], from_far.at[here], send_sem.at[part, 2],
                            recv_sem.at[part, 2], peer("tensor", far)))
    for copy in first:
        copy.start()
    if with_side:
        side_near, side_buf, side_far, side_send, side_recv = rest[5:]
        srows = side_out.shape[0]

        def side_block(index):
            return pl.ds(pl.multiple_of(index * srows, 8), srows)

        s1 = remote(side_ref.at[side_block(cross)], side_near.at[0], side_send.at[0], side_recv.at[0], peer("tensor", near))
        s2 = remote(side_ref.at[side_block(near)], side_near.at[1], side_send.at[1], side_recv.at[1], peer("tensor", near))
        s3 = remote(side_buf, side_far, side_send.at[2], side_recv.at[2], peer("tensor", far))
        s1.start()
        s2.start()
    for copy in second:
        copy.start()
    if with_side:
        s1.wait_recv()
        side_buf[...] = side_ref[side_block(far), :] + side_near[0]
        s3.start()
    for part in range(RS_PIECES):
        here = pl.ds(part * size, size)
        first[part].wait_recv()
        to_far_buf[here, :] = (
            value_ref[block(far, part), :].astype(F32) + from_near[0, here, :].astype(F32)
        ).astype(to_far_buf.dtype)
        third[part].start()
    if with_side:
        s2.wait_recv()
        s3.wait_recv()
        side_out[...] = side_ref[side_block(me), :] + side_near[1] + side_far[...]
        s1.wait_send()
        s2.wait_send()
        s3.wait_send()
    for part in range(RS_PIECES):
        here = pl.ds(part * size, size)
        second[part].wait_recv()
        out_ref[here, :] = value_ref[block(me, part), :].astype(F32) + from_near[1, here, :].astype(F32)
    for part in range(RS_PIECES):
        here = pl.ds(part * size, size)
        third[part].wait_recv()
        out_ref[here, :] = out_ref[here, :] + from_far[here, :].astype(F32)
    for copy in first + second + third:
        copy.wait_send()


def token_scatter(value, group_id, side=None):
    n = lax.axis_size("tensor")
    rows, cols = value.shape[0] // n, value.shape[1]
    operands = [value]
    out_shape = [jax.ShapeDtypeStruct((rows, cols), F32)]
    scratch = [
        pltpu.VMEM((2, rows, cols), value.dtype),
        pltpu.VMEM((rows, cols), value.dtype),
        pltpu.VMEM((rows, cols), value.dtype),
        pltpu.SemaphoreType.DMA((RS_PIECES, 3)),
        pltpu.SemaphoreType.DMA((RS_PIECES, 3)),
    ]
    if side is not None:
        srows, scols = side.shape[0] // n, side.shape[1]
        operands.append(side)
        out_shape.append(jax.ShapeDtypeStruct((srows, scols), F32))
        scratch += [
            pltpu.VMEM((2, srows, scols), F32),
            pltpu.VMEM((srows, scols), F32),
            pltpu.VMEM((srows, scols), F32),
            pltpu.SemaphoreType.DMA((3,)),
            pltpu.SemaphoreType.DMA((3,)),
        ]
    return pl.pallas_call(
        functools.partial(token_scatter_kernel, side is not None),
        out_shape=out_shape,
        in_specs=[pl.BlockSpec(memory_space=pltpu.VMEM)] * len(operands),
        out_specs=[pl.BlockSpec(memory_space=pltpu.VMEM)] * len(operands),
        scratch_shapes=scratch,
        cost_estimate=cost(22),
        compiler_params=pltpu.CompilerParams(collective_id=group_id, has_side_effects=True, vmem_limit_bytes=40 << 20),
        name="token_scatter",
    )(*operands)


def open_kernel(n, pieces, in_ref, out_ref, xn_ref, fin_ref, fout_ref, xall_ref,
                x_ss, x_rs, z_ss, z_rs, own_sem, t_ss, t_rs):
    sec, z, ten = lax.axis_index("section"), lax.axis_index("dp"), lax.axis_index("tensor")
    across = peer("section", 1 - sec)
    near, far = peer("tensor", ten ^ 1), peer("tensor", ten ^ 2)
    barrier = pltpu.get_barrier_semaphore()
    for where in (across, near, far):
        pl.semaphore_signal(barrier, inc=1, device_id=where, device_id_type=MESH_ID)

    @pl.when(z > 0)
    def _():
        pl.semaphore_signal(barrier, inc=1, device_id=peer("dp", z - 1), device_id_type=MESH_ID)

    @pl.when(z < n - 1)
    def _():
        pl.semaphore_signal(barrier, inc=1, device_id=peer("dp", z + 1), device_id_type=MESH_ID)

    pl.semaphore_wait(barrier, 3 + jnp.where(z > 0, 1, 0) + jnp.where(z < n - 1, 1, 0))
    sources, fulls = (in_ref, out_ref), (fin_ref, fout_ref)
    rows = in_ref.shape[0]
    trows = xn_ref.shape[0]

    def place(p, s):
        array, offset, count, _ = pieces[p]
        return fulls[array].at[pl.ds(pl.multiple_of(s * rows + offset, 16), count)]

    def own(p):
        array, offset, count, _ = pieces[p]
        return sources[array].at[pl.ds(offset, count)]

    def to_x(p, s, source):
        return remote(source, place(p, s), x_ss.at[p, s], x_rs.at[p, s], across)

    def to_z(p, s, step, source):
        side = 0 if step > 0 else 1
        return remote(source, place(p, s), z_ss.at[side, p, s], z_rs.at[side, p, s], peer("dp", z + step))

    def got_z(p, s, side):
        remote(own(p), place(p, s), z_ss.at[side, p, 0], z_rs.at[side, p, s], across).wait_recv()

    def spread(p, s, source, right=True, left=True):
        if right:
            @pl.when(z < n - 1)
            def _():
                to_z(p, s, 1, source).start()
        if left:
            @pl.when(z > 0)
            def _():
                to_z(p, s, -1, source).start()

    every = range(len(pieces))
    via = [piece[3] for piece in pieces]
    me = pl.ds(pl.multiple_of(ten * trows, 16), trows)
    other = pl.ds(pl.multiple_of((ten ^ 2) * trows, 16), trows)
    tok_far = remote(xn_ref, xall_ref.at[me], t_ss.at[0], t_rs.at[0], far)
    tok_near = remote(xn_ref, xall_ref.at[me], t_ss.at[1], t_rs.at[1], near)
    tok_relay = remote(xall_ref.at[other], xall_ref.at[other], t_ss.at[2], t_rs.at[2], near)
    tok_own = pltpu.make_async_copy(xn_ref, xall_ref.at[me], own_sem.at[0])
    tok_far.start()
    tok_near.start()
    tok_own.start()

    @pl.when(sec == 0)
    def _():
        for p in every:
            if via[p] == 1:
                to_x(p, z, own(p)).start()
            else:
                spread(p, z, own(p))
        for p in every:
            if via[p] == 0:
                to_x(p, z, own(p)).start()
        for array in (0, 1):
            whole = fulls[array].at[pl.ds(pl.multiple_of(z * rows, 16), rows)]
            pltpu.make_async_copy(sources[array], whole, own_sem.at[1 + array]).start()
        for d in range(1, n):
            for p in every:
                if via[p] == 0:
                    @pl.when(z - d >= 0)
                    def _():
                        got_z(p, z - d, 0)
                        spread(p, z - d, place(p, z - d), left=False)
                        to_x(p, z - d, place(p, z - d)).start()

                    @pl.when(z + d < n)
                    def _():
                        got_z(p, z + d, 1)
                        spread(p, z + d, place(p, z + d), right=False)
                        to_x(p, z + d, place(p, z + d)).start()
        for d in range(1, n):
            s = lax.rem(z + d, n)
            for p in every:
                if via[p] == 1:
                    to_x(p, s, place(p, s)).wait_recv()

    @pl.when(sec == 1)
    def _():
        for p in every:
            if via[p] == 1:
                to_x(p, z, place(p, z)).wait_recv()
                spread(p, z, place(p, z))
        for d in range(1, n):
            for p in every:
                if via[p] == 1:
                    @pl.when(z - d >= 0)
                    def _():
                        got_z(p, z - d, 0)
                        spread(p, z - d, place(p, z - d), left=False)
                        to_x(p, z - d, place(p, z - d)).start()

                    @pl.when(z + d < n)
                    def _():
                        got_z(p, z + d, 1)
                        spread(p, z + d, place(p, z + d), right=False)
                        to_x(p, z + d, place(p, z + d)).start()
        for d in range(n):
            s = lax.rem(z + d, n)
            for p in every:
                if via[p] == 0:
                    to_x(p, s, place(p, s)).wait_recv()

    tok_far.wait_recv()
    tok_relay.start()
    tok_near.wait_recv()
    tok_relay.wait_recv()
    for copy in (tok_far, tok_near, tok_relay):
        copy.wait_send()
    tok_own.wait()

    @pl.when(sec == 0)
    def _():
        for array in (0, 1):
            whole = fulls[array].at[pl.ds(pl.multiple_of(z * rows, 16), rows)]
            pltpu.make_async_copy(sources[array], whole, own_sem.at[1 + array]).wait()

    for p in every:
        for d in range(n):
            s = lax.rem(z + d, n)
            mine = sec == via[p]
            if d == 0:
                sent_x = jnp.logical_or(sec == 0, False)
            else:
                sent_x = mine

            @pl.when(sent_x)
            def _():
                to_x(p, s, place(p, s)).wait_send()

            @pl.when(mine & (s <= z) & (z < n - 1))
            def _():
                to_z(p, s, 1, place(p, s)).wait_send()

            @pl.when(mine & (s >= z) & (z > 0))
            def _():
                to_z(p, s, -1, place(p, s)).wait_send()


def open_gather(own_in, own_out, xn, group_id):
    n = lax.axis_size("dp")
    rows = own_in.shape[0]
    third = rows // 3
    pieces = (
        (0, third, third, 1), (0, 2 * third, third, 1), (0, 0, third, 0),
        (1, third, 2 * third, 1), (1, 0, third, 0),
    )
    count = len(pieces)
    sem = lambda *shape: pltpu.SemaphoreType.DMA(shape)
    return pl.pallas_call(
        functools.partial(open_kernel, n, pieces),
        out_shape=[
            jax.ShapeDtypeStruct((n * rows, own_in.shape[1]), BF),
            jax.ShapeDtypeStruct((n * rows, own_out.shape[1]), BF),
            jax.ShapeDtypeStruct((lax.axis_size("tensor") * xn.shape[0], xn.shape[1]), BF),
        ],
        in_specs=[pl.BlockSpec(memory_space=pltpu.VMEM)] * 3,
        out_specs=[pl.BlockSpec(memory_space=pl.ANY)] * 3,
        scratch_shapes=[sem(count, n), sem(count, n), sem(2, count, n), sem(2, count, n), sem(3), sem(3), sem(3)],
        cost_estimate=cost(110),
        compiler_params=pltpu.CompilerParams(collective_id=group_id, has_side_effects=True),
        name="weights_open",
    )(own_in, own_out, xn)


CHUNK_ROWS = 16


def by_rows(count, body):
    @pl.loop(0, count // CHUNK_ROWS)
    def _(index):
        body(pl.multiple_of(index * CHUNK_ROWS, CHUNK_ROWS))


def finish_kernel(
    n, bc_at, gain_rows,
    g_ref, mid_ref, half_ref, own_ref, gp_ref, w_ref, u_ref, seed_ref, inv_ref, gain_ref, small_ref,
    gin_ref, gout_ref, small_x_ref, small_t_ref, bc_ref, du_ref, du_got_ref,
    x_recv, z_recv, z_send, o_recv, o_send, last_buf, last_recv, join_recv, olast_buf, olast_recv,
    part_a, part_b, near_recv, far_send, far_recv, dxn, gain_acc,
    small_own, small_recv, small_all, small_ten, bc_own, bc_far, bc_mid, bc_near,
    x_ss, x_rs, z_ss, z_rs, o_ss, o_rs, m_ss, m_rs, d_ss, d_rs, t_ss, t_rs, y_ss, y_rs,
):
    sec, z, ten = lax.axis_index("section"), lax.axis_index("dp"), lax.axis_index("tensor")
    half, wide = half_ref.shape
    rows = 2 * half
    mine, theirs = sec * half, (1 - sec) * half
    across = peer("section", 1 - sec)
    near, far = peer("tensor", ten ^ 1), peer("tensor", ten ^ 2)
    others = [lax.rem(z + d, n) for d in range(1, n)]
    mates = [ten ^ d for d in range(1, 4)]
    greet([across] + [peer("dp", o) for o in others] + [peer("tensor", t) for t in mates])
    cut = wide // 256 * 128
    columns = (slice(cut, wide), slice(0, cut))
    order = [i // 2 if i % 2 else n - 1 - i // 2 for i in range(n)]

    def shard_rows(s, offset):
        return pl.ds(pl.multiple_of(s * rows + offset, 16), half)

    x_copies = {}
    for c, cols in enumerate(columns):
        for s in order:
            x_copies[c, s] = remote(
                g_ref.at[shard_rows(s, theirs), cols], x_recv.at[s, :, cols], x_ss.at[c, s], x_rs.at[c, s], across
            )
    early = [(0, s) for s in order] + [(1, order[0])]
    for key in early:
        x_copies[key].start()
    join = remote(half_ref, join_recv, m_ss.at[0], m_rs.at[0], across)
    ojoin = remote(own_ref, olast_recv, m_ss.at[1], m_rs.at[1], across)
    olast = remote(olast_buf, olast_recv, m_ss.at[1], m_rs.at[1], across)
    lasts = [
        remote(last_buf.at[:, cols], last_recv.at[:, cols], m_ss.at[2 + c], m_rs.at[2 + c], across)
        for c, cols in enumerate(columns)
    ]
    du_copy = remote(du_ref, du_got_ref, m_ss.at[4], m_rs.at[4], across)

    @pl.when(sec == 0)
    def _():
        ojoin.start()

    trows = u_ref.shape[0]
    step = 256
    tiles = w_ref.shape[0] // step

    def product(index, put):
        @pl.loop(0, tiles)
        def _(tile):
            at = pl.ds(pl.multiple_of(tile * step, step), step)
            put(at, dot_nt(gp_ref[pl.ds(pl.multiple_of(index * trows, 16), trows), :], w_ref[at, :]))

    y_cross = remote(part_a, near_recv.at[0], y_ss.at[0], y_rs.at[0], near)
    y_near = remote(part_b, near_recv.at[1], y_ss.at[1], y_rs.at[1], near)
    y_far = remote(far_send, far_recv, y_ss.at[2], y_rs.at[2], far)

    def put_a(at, value):
        part_a[:, at] = value.astype(BF)

    def put_b(at, value):
        part_b[:, at] = value.astype(BF)

    def put_far(at, value):
        far_send[:, at] = (value + near_recv[0, :, at].astype(F32)).astype(BF)

    def put_own(at, value):
        dxn[:, at] = value

    product(ten ^ 3, put_a)
    y_cross.start()
    product(ten ^ 1, put_b)
    y_near.start()
    y_cross.wait_recv()
    product(ten ^ 2, put_far)
    y_far.start()
    product(ten, put_own)

    def down(s):
        right = s > z
        return jnp.where(right, 0, 1), peer("dp", z + jnp.where(right, 1, -1)), jnp.where(right, z > 0, z < n - 1)

    def reduce_step(s, plain, recv, send, ss, rs, cols):
        @pl.when(s != z)
        def _():
            side, below, upstream = down(s)

            @pl.when(upstream)
            def _():
                remote(send.at[s, :, cols], recv.at[side, s, :, cols], ss.at[s], rs.at[side, s], across).wait_recv()

                def body(r):
                    at = pl.ds(r, CHUNK_ROWS)
                    send[s, at, cols] = (plain(s, r, cols) + recv[side, s, at, cols].astype(F32)).astype(BF)

                by_rows(half, body)

            @pl.when(jnp.logical_not(upstream))
            def _():
                def body(r):
                    send[s, pl.ds(r, CHUNK_ROWS), cols] = plain(s, r, cols).astype(BF)

                by_rows(half, body)

            remote(send.at[s, :, cols], recv.at[side, s, :, cols], ss.at[s], rs.at[side, s], below).start()

    def reduce_own(plain, recv, ss, rs, send, cols, target):
        def base(r):
            target[pl.ds(r, CHUNK_ROWS), cols] = plain(z, r, cols)

        by_rows(half, base)
        for side, there in ((0, z > 0), (1, z < n - 1)):

            @pl.when(there)
            def _():
                remote(send.at[0, :, cols], recv.at[side, z, :, cols], ss.at[0], rs.at[side, z], across).wait_recv()

                def more(r):
                    at = pl.ds(r, CHUNK_ROWS)
                    target[at, cols] += recv[side, z, at, cols].astype(F32)

                by_rows(half, more)

    def reduce_done(send, recv, ss, rs, cols):
        for s in order:
            @pl.when(s != z)
            def _():
                side, below, _ = down(s)
                remote(send.at[s, :, cols], recv.at[side, s, :, cols], ss.at[s], rs.at[side, s], below).wait_send()

    def in_plain(s, r, cols):
        at = pl.ds(pl.multiple_of(s * rows + mine + r, 16), CHUNK_ROWS)
        return g_ref[at, cols].astype(F32) + x_recv[s, pl.ds(r, CHUNK_ROWS), cols].astype(F32)

    def out_plain(s, r, cols):
        return mid_ref[pl.ds(pl.multiple_of(s * half + r, 16), CHUNK_ROWS), cols].astype(F32)

    ocols = slice(0, own_ref.shape[1])

    def in_step(c, k):
        s = order[k]
        x_copies[c, s].wait_recv()
        reduce_step(s, in_plain, x_in, z_in, z_ss.at[c], z_rs.at[c], columns[c])

    x_in, z_in = z_recv, z_send
    for s in order:
        reduce_step(s, out_plain, o_recv, o_send, o_ss, o_rs, ocols)
    in_step(0, 0)
    in_step(0, 1)
    y_near.wait_recv()
    y_far.wait_recv()
    gain_acc[...] = jnp.zeros_like(gain_acc)
    model = u_ref.shape[1]

    def du_rows(r):
        at = pl.ds(r, CHUNK_ROWS)
        u = u_ref[at, :].astype(F32)
        inv = inv_ref[at, :]
        grad = dxn[at, :] + near_recv[1, at, :].astype(F32) + far_recv[at, :].astype(F32)
        scaled = grad * gain_ref[...]
        dots = jnp.sum(scaled * u, axis=1, keepdims=True)
        du_ref[at, :] = (seed_ref[at, :].astype(F32) + inv * scaled - u * (inv * inv * inv * dots / model)).astype(BF)
        gain_acc[...] += fold8(grad * u * inv)

    by_rows(trows, du_rows)

    srows, swide = small_recv.shape
    small_own[...] = small_ref[...]
    gain_sum = jnp.sum(gain_acc[...], axis=0, keepdims=True)
    for k in range(gain_rows):
        part = gain_sum[:, k * swide : min((k + 1) * swide, model)]
        small_own[8 + k : 9 + k, 0 : part.shape[1]] = part
    small_x = remote(small_own.at[pl.ds(pl.multiple_of((1 - sec) * srows, 8), srows)], small_recv,
                     m_ss.at[5], m_rs.at[5], across)
    small_x.start()
    for key, copy in x_copies.items():
        if key not in early:
            copy.start()

    @pl.when(sec == 1)
    def _():
        du_copy.start()

    @pl.when(sec == 0)
    def _():
        join.start()

    for k in range(2, n):
        in_step(0, k)
    small_x.wait_recv()
    small_all[z] = small_own[pl.ds(pl.multiple_of(sec * srows, 8), srows), :] + small_recv[...]
    to_dp = [remote(small_all.at[z], small_all.at[z], d_ss.at[d], d_rs.at[z], peer("dp", o)) for d, o in enumerate(others)]
    for copy in to_dp:
        copy.start()
    reduce_own(out_plain, o_recv, o_ss, o_rs, o_send, ocols, gout_ref)

    def halves(own_part, got, target, cols, own_first):
        def put(r):
            at, low = pl.ds(r, CHUNK_ROWS), pl.ds(pl.multiple_of(half + r, 16), CHUNK_ROWS)
            if own_first:
                target[low, cols] = got[at, cols].astype(F32)
            else:
                target[at, cols] = got[at, cols].astype(F32)
                target[low, cols] = own_part[at, cols].astype(F32)

        by_rows(half, put)

    def hand_over(target, buffer, cols):
        def put(r):
            at = pl.ds(r, CHUNK_ROWS)
            buffer[at, cols] = target[at, cols].astype(BF)

        by_rows(half, put)

    @pl.when(sec == 1)
    def _():
        hand_over(gout_ref, olast_buf, ocols)
        olast.start()

    def start_bc():
        bc_own[...] = gin_ref[:, bc_at : bc_at + 2 * NS].astype(BF)
        remote(bc_own, bc_far, t_ss.at[3], t_rs.at[4], far).start()

    for c, cols in enumerate(columns):
        if c:
            for k in range(n):
                in_step(c, k)
            for d, o in enumerate(others):
                remote(small_all.at[o], small_all.at[o], d_ss.at[d], d_rs.at[o], across).wait_recv()
            total = small_all[0]
            for k in range(1, n):
                total = total + small_all[k]
            small_x_ref[...] = total
            small_ten[ten] = total
            to_ten = [
                remote(small_ten.at[ten], small_ten.at[ten], t_ss.at[d], t_rs.at[ten], peer("tensor", t))
                for d, t in enumerate(mates)
            ]
            for copy in to_ten:
                copy.start()
        reduce_own(in_plain, x_in, z_ss.at[c], z_rs.at[c], z_in, cols, gin_ref)

        @pl.when(sec == 1)
        def _():
            hand_over(gin_ref, last_buf, cols)
            lasts[c].start()

    @pl.when(sec == 1)
    def _():
        olast.wait_recv()
        halves(own_ref, olast_recv, gout_ref, ocols, False)
        join.wait_recv()
        for cols in columns:
            halves(half_ref, join_recv, gin_ref, cols, False)
        start_bc()

    @pl.when(sec == 0)
    def _():
        lasts[0].wait_recv()
        halves(None, last_recv, gin_ref, columns[0], True)
        start_bc()
        olast.wait_recv()
        halves(None, olast_recv, gout_ref, ocols, True)
        lasts[1].wait_recv()
        halves(None, last_recv, gin_ref, columns[1], True)
        du_copy.wait_recv()
        ojoin.wait_send()
        join.wait_send()

    for d, t in enumerate(mates):
        remote(small_ten.at[t], small_ten.at[t], t_ss.at[d], t_rs.at[t], near).wait_recv()
    total = small_ten[0]
    for k in range(1, 4):
        total = total + small_ten[k]
    small_t_ref[...] = total
    to_far = remote(bc_own, bc_far, t_ss.at[3], t_rs.at[4], far)
    to_far.wait_recv()
    bc_mid[...] = (bc_own[...].astype(F32) + bc_far[...].astype(F32)).astype(BF)
    to_near = remote(bc_mid, bc_near, t_ss.at[4], t_rs.at[5], near)
    to_near.start()
    to_near.wait_recv()
    bc_ref[...] = bc_mid[...].astype(F32) + bc_near[...].astype(F32)
    for c, cols in enumerate(columns):
        for s in order:
            x_copies[c, s].wait_send()
        reduce_done(z_in, x_in, z_ss.at[c], z_rs.at[c], cols)
    reduce_done(o_send, o_recv, o_ss, o_rs, ocols)

    @pl.when(sec == 1)
    def _():
        olast.wait_send()
        for copy in lasts:
            copy.wait_send()
        du_copy.wait_send()

    for copy in [small_x, to_far, to_near, y_cross, y_near, y_far] + to_dp + to_ten:
        copy.wait_send()


def finish(grads, out_mid, half_other, out_other, gp, w_in, u, seed, inv, gain, smalls, bc_at, gain_rows, group_id):
    n = lax.axis_size("dp")
    half, wide = half_other.shape
    owide = out_other.shape[1]
    trows, model = u.shape
    srows, swide = smalls.shape[0] // 2, smalls.shape[1]
    vm = lambda dtype, *shape: pltpu.VMEM(shape, dtype)
    sem = lambda *shape: pltpu.SemaphoreType.DMA(shape)
    return pl.pallas_call(
        functools.partial(finish_kernel, n, bc_at, gain_rows),
        out_shape=[
            jax.ShapeDtypeStruct((2 * half, wide), F32),
            jax.ShapeDtypeStruct((2 * half, owide), F32),
            jax.ShapeDtypeStruct((srows, swide), F32),
            jax.ShapeDtypeStruct((srows, swide), F32),
            jax.ShapeDtypeStruct((2 * half, 2 * NS), F32),
            jax.ShapeDtypeStruct((trows, model), BF),
            jax.ShapeDtypeStruct((trows, model), BF),
        ],
        in_specs=[pl.BlockSpec(memory_space=pltpu.VMEM)] * 11,
        out_specs=[pl.BlockSpec(memory_space=pltpu.VMEM)] * 7,
        scratch_shapes=[
            vm(BF, n, half, wide), vm(BF, 2, n, half, wide), vm(BF, n, half, wide),
            vm(BF, 2, n, half, owide), vm(BF, n, half, owide),
            vm(BF, half, wide), vm(BF, half, wide), vm(BF, half, wide), vm(BF, half, owide), vm(BF, half, owide),
            vm(BF, trows, model), vm(BF, trows, model), vm(BF, 2, trows, model), vm(BF, trows, model),
            vm(BF, trows, model), vm(F32, trows, model), vm(F32, 8, model),
            vm(F32, 2 * srows, swide), vm(F32, srows, swide), vm(F32, n, srows, swide), vm(F32, 4, srows, swide),
            vm(BF, 2 * half, 2 * NS), vm(BF, 2 * half, 2 * NS), vm(BF, 2 * half, 2 * NS), vm(BF, 2 * half, 2 * NS),
            sem(2, n), sem(2, n), sem(2, n), sem(2, 2, n), sem(n), sem(2, n),
            sem(6), sem(6), sem(n), sem(n), sem(5), sem(6), sem(3), sem(3),
        ],
        cost_estimate=cost(120),
        compiler_params=pltpu.CompilerParams(collective_id=group_id, has_side_effects=True, vmem_limit_bytes=63 << 20),
        name="grad_finish",
    )(grads, out_mid, half_other, out_other, gp, w_in, u, seed, inv, gain, smalls)


EPSILON = 1e-05
HEAD_PAD = 128
SMALL_ROWS = 16


def swap_sections(value):
    count = lax.axis_size("section")
    return lax.ppermute(value, "section", [(i, (i + 1) % count) for i in range(count)])


def later_gather(own, is_first, after):
    half = own.shape[0] // 2
    low, high = own[:half], own[half:]
    got = lax.ppermute(low, "section", [(1, 0)])
    piece, after = lax.optimization_barrier((jnp.where(is_first, got, high), after))
    return lax.all_gather(piece, ("dp", "section"), axis=0, tiled=True), after


def grad_scatter(value):
    return lax.psum_scatter(value, ("dp", "section"), scatter_dimension=0, tiled=True)


def local(
    stream, cotangent, norm_gain, in_zx, in_dt, in_bc, out_proj, conv_x, conv_x_bias,
    conv_bc, conv_bc_bias, dt_bias, a_log, d_skip, gate_gain,
):
    section = lax.axis_index("section")
    is_first = section == 0
    model = stream.shape[3]
    rows = stream.shape[2]
    width = conv_x.shape[2]
    heads = dt_bias.shape[1]
    shard = in_zx.shape[1]
    total_inner = width * lax.axis_size("tensor")
    wide = width + 2 * NS

    def padded(value):
        return jnp.pad(value, (0, wide - value.shape[0]))[None]

    gain_rows = -(-model // wide)
    own_par = jnp.concatenate(
        [
            jnp.concatenate([conv_x[0], conv_bc[0]], axis=1),
            jnp.concatenate([conv_x_bias[0], conv_bc_bias[0]])[None],
            padded(gate_gain[0]),
            padded(jnp.repeat(d_skip[0], width // heads)),
            padded(dt_bias[0]),
            padded(a_log[0]),
            jnp.pad(norm_gain[0], (0, gain_rows * wide - model)).reshape(gain_rows, wide),
            jnp.zeros((7 - gain_rows, wide), F32),
        ],
        axis=0,
    )
    other_par = swap_sections(own_par)
    pars = (jnp.where(is_first, own_par, other_par), jnp.where(is_first, other_par, own_par))
    gains = tuple(par[9 : 9 + gain_rows].reshape(-1)[:model] for par in pars)

    own_in = jnp.concatenate(
        [
            in_zx[0].reshape(shard, 2 * width),
            in_bc[0],
            jnp.pad(in_dt[0], ((0, 0), (0, HEAD_PAD - heads))),
        ],
        axis=1,
    )
    own_out = out_proj[0].T

    head_of = jnp.arange(width) // (width // heads)
    spread = (jnp.arange(2 * HEAD_PAD)[:, None] % HEAD_PAD == head_of[None, :]).astype(BF)
    gather = (head_of[:, None] == jnp.arange(HEAD_PAD)[None, :]).astype(BF)

    def normed(layer, u):
        inv = lax.rsqrt(jnp.mean(u * u, axis=1, keepdims=True) + EPSILON)
        return inv, (u * inv * gains[layer][None, :]).astype(BF)

    def forward(layer, u, inv, xn, w_in, w_out):
        pre = dot(xn, w_in)
        yn, squares, states = mixer_fwd(pre, pars[layer], spread, width)
        partial = dot_nt(yn, w_out).astype(BF)
        total, squares = token_scatter(partial, 3 + layer, squares)
        q = lax.rsqrt(squares[::8].reshape(rows) / total_inner + EPSILON)[:, None]
        projected = total * q
        return (u + projected).astype(BF), (u, inv, xn, pre, yn, states, q, projected, w_in, w_out)

    def backward_core(layer, g, kept):
        u, inv, xn, pre, yn, states, q, projected, w_in, w_out = kept
        kappa = q * q / total_inner * jnp.sum(g * projected, axis=1, keepdims=True)
        high = kappa.astype(BF)
        low = (kappa - high.astype(F32)).astype(BF)
        side = jnp.pad(jnp.concatenate([high, low], axis=1), ((0, 0), (0, 126)))
        gq, side = token_gather([(g * q).astype(BF), side], 5 + layer)
        g_out = dot_tn(gq, yn).astype(BF)
        dh = dot(gq, w_out)
        gp, acc = mixer_bwd(pre, pars[layer], spread, gather, states, dh, side, width, heads)
        g_in = dot_tn(xn, gp).astype(BF)
        return gp, acc, g_in, g_out

    def backward_input(layer, g, kept, gp):
        u, inv = kept[:2]
        (dxn,) = token_scatter(dot_nt(gp, kept[8]).astype(BF), 7 + layer)
        scaled = dxn * gains[layer][None, :]
        dots = jnp.sum(scaled * u, axis=1, keepdims=True)
        du = g + inv * scaled - u * (inv * inv * inv) * dots / model
        return du.astype(BF), jnp.sum(dxn * u * inv, axis=0)

    stream_own = lax.dynamic_index_in_dim(stream[:, 0], section, 0, False)
    u0 = stream_own.astype(F32)
    inv0, xn0 = normed(0, u0)
    w_in0, w_out0, xn0 = open_gather(own_in, own_out, xn0, 1)
    full_in1, w_in0 = later_gather(own_in, is_first, w_in0)
    full_out1, w_in0 = later_gather(own_out, is_first, w_in0)

    out0, kept0 = forward(0, u0, inv0, xn0, w_in0, w_out0)
    u1 = out0.astype(F32)
    inv1, xn1 = normed(1, u1)
    (xn1,) = token_gather([xn1], 2)
    out1, kept1 = forward(1, u1, inv1, xn1, full_in1, full_out1)
    g1 = lax.dynamic_index_in_dim(cotangent[:, 0], section, 0, False).astype(F32)
    gp1, acc1, g_in1, g_out1 = backward_core(1, g1, kept1)
    half_out1 = grad_scatter(g_out1)
    half_in1 = grad_scatter(g_in1)
    gp1, g_in1 = lax.optimization_barrier((gp1, g_in1))
    du1, gain1 = backward_input(1, g1, kept1, gp1)
    gp0, acc0, g_in0, g_out0 = backward_core(0, du1.astype(F32), kept0)
    split_out = g_out0.reshape(-1, 2, shard // 2, width)
    mine = jnp.where(is_first, split_out[:, 0], split_out[:, 1])
    theirs = swap_sections(jnp.where(is_first, split_out[:, 1], split_out[:, 0]))
    out_mid = (mine.astype(F32) + theirs.astype(F32)).astype(BF).reshape(-1, width)
    du1_first = lax.ppermute(du1, "section", [(0, 1)])

    def by_batch(first_value, second_value):
        own = jnp.where(is_first, first_value, second_value)
        got = swap_sections(jnp.where(is_first, second_value, first_value))
        stacked = jnp.stack([jnp.where(is_first, own, got), jnp.where(is_first, got, own)])
        return stacked[None, :, None]

    def minor(acc, gain):
        return jnp.concatenate(
            [
                acc,
                jnp.pad(gain, (0, gain_rows * wide - model)).reshape(gain_rows, wide),
                jnp.zeros((SMALL_ROWS - 8 - gain_rows, wide), F32),
            ],
            axis=0,
        )

    smalls = jnp.concatenate([minor(acc0, jnp.zeros_like(gain1)), minor(acc1, gain1)])
    g_in, g_out, mine, shared, bc_rows, du0, du0_second = finish(
        g_in0, out_mid, half_in1, half_out1, gp0, w_in0, stream_own, du1, inv0, gains[0][None, :],
        smalls, 2 * width, gain_rows, 9,
    )
    grads = jnp.stack([jnp.where(is_first, du0, du1_first), jnp.where(is_first, du0_second, du1)])
    return (
        by_batch(out0, out1),
        grads[None, :, None],
        shared[8 : 8 + gain_rows].reshape(-1)[:model][None],
        g_in[:, : 2 * width].reshape(shard, 2, width)[None],
        g_in[:, 2 * width + 2 * NS : 2 * width + 2 * NS + heads][None],
        bc_rows[None],
        g_out.T[None],
        mine[0:4, :width][None],
        mine[4, :width][None],
        shared[0:4, width:][None],
        shared[4, width:][None],
        mine[7, :heads][None],
        mine[7, HEAD_PAD : HEAD_PAD + heads][None],
        mine[6, :width].reshape(heads, -1).sum(axis=1)[None],
        mine[5, :width][None],
    )


def solution(mesh):
    in_specs = (
        P(None, "dp", "tensor", None),
        P(None, "dp", "tensor", None),
        P("section", None),
        P("section", "dp", None, "tensor"),
        P("section", "dp", "tensor"),
        P("section", "dp", None),
        P("section", "tensor", "dp"),
        P("section", None, "tensor"),
        P("section", "tensor"),
        P("section", None, None),
        P("section", None),
        P("section", "tensor"),
        P("section", "tensor"),
        P("section", "tensor"),
        P("section", "tensor"),
    )
    out_specs = (
        P("section", None, "dp", "tensor", None),
        P("section", None, "dp", "tensor", None),
        P("section", None),
        P("section", "dp", None, "tensor"),
        P("section", "dp", "tensor"),
        P("section", "dp", None),
        P("section", "tensor", "dp"),
        P("section", None, "tensor"),
        P("section", "tensor"),
        P("section", None, None),
        P("section", None),
        P("section", "tensor"),
        P("section", "tensor"),
        P("section", "tensor"),
        P("section", "tensor"),
    )
    return jax.shard_map(local, mesh=mesh, in_specs=in_specs, out_specs=out_specs, check_vma=False)
```

```python
import functools

import jax
import jax.numpy as jnp
from jax import lax
from jax.sharding import PartitionSpec as P
from jax.experimental import pallas as pl
from jax.experimental.pallas import tpu as pltpu

BF = jnp.bfloat16
F32 = jnp.float32
NS = 128
Q = 128
CONV = 4


def cost(us):
    return pl.CostEstimate(flops=us * 700_000_000, bytes_accessed=us * 1_500_000, transcendentals=0)


def dot(a, b):
    return jnp.dot(a, b, preferred_element_type=F32)


def dot_nt(a, b):
    return lax.dot_general(a, b, (((1,), (1,)), ((), ())), preferred_element_type=F32)


def dot_tn(a, b):
    return lax.dot_general(a, b, (((0,), (0,)), ((), ())), preferred_element_type=F32)


def dot_hi(a, b):
    return lax.dot_general(
        a, b, (((1,), (0,)), ((), ())), preferred_element_type=F32, precision=lax.Precision.HIGHEST
    )


def fold8(v):
    return jnp.sum(v.reshape(v.shape[0] // 8, 8, v.shape[1]), axis=0)


def expand(v, spread_ref):
    hi = v.astype(BF)
    lo = (v - hi.astype(F32)).astype(BF)
    return dot(jnp.concatenate([hi, lo], axis=1), spread_ref[...])


def head_rows(pre_ref, par_ref, width):
    raw = pre_ref[:, 2 * width + 2 * NS :] + par_ref[7:8, :NS]
    dt = jnp.maximum(raw, 0.0) + jnp.log1p(jnp.exp(-jnp.abs(raw)))
    rate = -jnp.exp(par_ref[8:9, :NS])
    row = lax.broadcasted_iota(jnp.int32, (Q, Q), 0)
    col = lax.broadcasted_iota(jnp.int32, (Q, Q), 1)
    return raw, dt, rate, row >= col


def split_heads(v, first):
    low = jnp.where(first, v, 0.0)
    return jnp.concatenate([low.astype(BF), (v - low).astype(BF)], axis=0)


def fwd_kernel(
    width, pre_ref, par_ref, spread_ref, yn_ref, sq_ref, st_ref, conv_ref, y_ref, ex_dt, ex_e, ex_w, cum_ref, cumt_ref, ext, state
):
    step = pl.program_id(0)
    pairs = width // 128

    @pl.when(step == 0)
    def _():
        ext[0:8, :] = jnp.zeros((8, ext.shape[1]), F32)
        state[...] = jnp.zeros_like(state)

    def conv_block(sl):
        at = slice(width + sl.start, width + sl.stop)
        ext[8:, sl] = pre_ref[:, at]
        conv = par_ref[4:5, sl] + par_ref[3:4, sl] * pre_ref[:, at]
        for k in range(CONV - 1):
            conv = conv + par_ref[k : k + 1, sl] * ext[5 + k : 5 + k + Q, sl]
        ext[0:8, sl] = pre_ref[Q - 8 : Q, at]
        conv_ref[:, sl] = conv
        return conv * jax.nn.sigmoid(conv)

    bm = conv_block(slice(width, width + NS)).astype(BF)
    cm = conv_block(slice(width + NS, width + 2 * NS)).astype(BF)
    raw, dt, rate, lower = head_rows(pre_ref, par_ref, width)
    cum = dot_hi(lower.astype(F32), dt * rate)
    cum_t = cum.T
    cum_ref[...] = cum
    cumt_ref[...] = cum_t
    ex_dt[...] = expand(dt, spread_ref)
    ex_e[...] = expand(jnp.exp(cum), spread_ref)
    ex_w[...] = expand(jnp.exp(cum[Q - 1 : Q, :] - cum), spread_ref)
    scores = dot_nt(cm, bm)
    st_ref[0] = state[...]
    bm_t = bm.T
    first = lax.broadcasted_iota(jnp.int32, (Q, 128), 1) < 64
    squares = jnp.zeros((Q, 128), F32)
    for p in range(pairs):
        sl = slice(128 * p, 128 * p + 128)
        x = conv_block(sl)
        xd = x * ex_dt[:, sl]
        st = state[:, sl]
        mixes = []
        for h in (2 * p, 2 * p + 1):
            gap = cum[:, h : h + 1] - cum_t[h : h + 1, :]
            mixes.append((jnp.exp(jnp.where(lower, gap, -1e30)) * scores).astype(BF))
        y = dot(jnp.concatenate(mixes, axis=1), split_heads(xd, first))
        y = y + ex_e[:, sl] * dot(cm, st.astype(BF)) + par_ref[6:7, sl] * x
        y_ref[:, sl] = y
        z = pre_ref[:, sl]
        yg = y * (z * jax.nn.sigmoid(z))
        squares = squares + yg * yg
        yn_ref[:, sl] = (yg * par_ref[5:6, sl]).astype(BF)
        state[:, sl] = ex_e[Q - 1 : Q, sl] * st + dot(bm_t, (ex_w[:, sl] * xd).astype(BF))
    sq_ref[...] = lax.dot_general(
        jnp.ones((8, 128), F32), squares, (((1,), (1,)), ((), ())),
        preferred_element_type=F32, precision=lax.Precision.HIGHEST,
    )


def mixer_fwd(pre, par, spread, width):
    T = pre.shape[0]
    n = T // Q
    pw = pre.shape[1]
    wide = width + 2 * NS
    return pl.pallas_call(
        functools.partial(fwd_kernel, width),
        grid=(n,),
        in_specs=[
            pl.BlockSpec((Q, pw), lambda i: (i, 0)),
            pl.BlockSpec(par.shape, lambda i: (0, 0)),
            pl.BlockSpec(spread.shape, lambda i: (0, 0)),
        ],
        out_specs=[
            pl.BlockSpec((Q, width), lambda i: (i, 0)),
            pl.BlockSpec((8, Q), lambda i: (i, 0)),
            pl.BlockSpec((1, NS, width), lambda i: (i, 0, 0)),
            pl.BlockSpec((Q, wide), lambda i: (i, 0)),
        ]
        + [pl.BlockSpec((Q, width), lambda i: (i, 0))] * 4
        + [pl.BlockSpec((Q, 128), lambda i: (i, 0))] * 2,
        out_shape=[
            jax.ShapeDtypeStruct((T, width), BF),
            jax.ShapeDtypeStruct((8 * n, Q), F32),
            jax.ShapeDtypeStruct((n, NS, width), F32),
            jax.ShapeDtypeStruct((T, wide), F32),
        ]
        + [jax.ShapeDtypeStruct((T, width), F32)] * 4
        + [jax.ShapeDtypeStruct((T, 128), F32)] * 2,
        scratch_shapes=[pltpu.VMEM((Q + 8, wide), F32), pltpu.VMEM((NS, width), F32)],
        compiler_params=pltpu.CompilerParams(dimension_semantics=("arbitrary",), vmem_limit_bytes=48 << 20),
        cost_estimate=cost(12),
        name="mixer_fwd",
    )(pre, par, spread)


def bwd_kernel(
    width, n_heads, pre_ref, par_ref, pick_ref, st_ref, conv_ref, y_ref, ex_dt, ex_e, ex_w, cum_ref, cumt_ref, dh_ref, kap_ref,
    gp_ref, acc_out, dext, dstate, acc,
):
    step = pl.program_id(0)
    steps = pl.num_programs(0)
    pairs = width // 128

    @pl.when(step == 0)
    def _():
        dext[Q:, :] = jnp.zeros((8, dext.shape[1]), F32)
        dstate[...] = jnp.zeros_like(dstate)
        acc[...] = jnp.zeros_like(acc)

    def activate(sl):
        conv = conv_ref[:, sl]
        sg = jax.nn.sigmoid(conv)
        act = conv * sg
        return act, sg + act * (1.0 - sg)

    def conv_back(sl, dact, slope):
        at = slice(width + sl.start, width + sl.stop)
        dconv = dact * slope
        pre = pre_ref[:, at]
        dext[0:Q, sl] = dconv
        dpre = par_ref[3:4, sl] * dconv
        acc[24:32, sl] += fold8(pre * dconv)
        acc[32:40, sl] += fold8(dconv)
        for k in range(CONV - 1):
            moved = dext[3 - k : 3 - k + Q, sl]
            dpre = dpre + par_ref[k : k + 1, sl] * moved
            acc[8 * k : 8 * k + 8, sl] += fold8(pre * moved)
        gp_ref[:, at] = dpre.astype(BF)
        dext[Q:, sl] = dconv[0:8, :]

    b_cols, c_cols = slice(width, width + NS), slice(width + NS, width + 2 * NS)
    bm, b_slope = activate(b_cols)
    cm, c_slope = activate(c_cols)
    bm, cm = bm.astype(BF), cm.astype(BF)
    raw, dt, rate, lower = head_rows(pre_ref, par_ref, width)
    cum, cum_t = cum_ref[...], cumt_ref[...]
    scores = dot_nt(cm, bm)
    cm_t = cm.T
    first = lax.broadcasted_iota(jnp.int32, (Q, 128), 1) < 64
    kap = kap_ref[:, 0:1].astype(F32) + kap_ref[:, 1:2].astype(F32)
    dscores = jnp.zeros((Q, Q), F32)
    sums = jnp.zeros((Q, 128), F32)
    cols = jnp.zeros((16, Q), F32)
    dC = jnp.zeros((Q, NS), F32)
    dB = jnp.zeros((Q, NS), F32)
    f_sum = jnp.zeros((8, 128), F32)
    crow = lax.broadcasted_iota(jnp.int32, (16, 2 * Q), 0)
    ccol = lax.broadcasted_iota(jnp.int32, (16, 2 * Q), 1)
    for p in range(pairs):
        sl = slice(128 * p, 128 * p + 128)
        x, slope = activate(sl)
        xdt = ex_dt[:, sl]
        xd = x * xdt
        xdb = xd.astype(BF)
        st = st_ref[0, :, sl]
        stb = st.astype(BF)
        decays, mixb = [], []
        for h in (2 * p, 2 * p + 1):
            gap = cum[:, h : h + 1] - cum_t[h : h + 1, :]
            decay = jnp.exp(jnp.where(lower, gap, -1e30))
            decays.append(decay)
            mixb.append((decay * scores).astype(BF))
        e = ex_e[:, sl]
        carried = e * dot(cm, stb)
        y = y_ref[:, sl]
        z = pre_ref[:, sl]
        sz = jax.nn.sigmoid(z)
        silz = z * sz
        yg = y * silz
        dh = dh_ref[:, sl]
        dyg = par_ref[5:6, sl] * dh - yg * kap
        acc[40:48, sl] += fold8(dh * yg)
        dy = dyg * silz
        gp_ref[:, sl] = (dyg * y * (sz + silz * (1.0 - sz))).astype(BF)
        acc[48:56, sl] += fold8(dy * x)
        dstack = split_heads(dy, first)
        dmix = dot_nt(dstack, xdb)
        rbs = []
        for j in range(2):
            part = decays[j] * dmix[Q * j : Q * j + Q]
            dscores = dscores + part
            rbs.append((part * scores).astype(BF))
        ones = (crow == 2 * p + (ccol >= Q).astype(jnp.int32)).astype(BF)
        cols = cols + dot(ones, jnp.concatenate(rbs, axis=0))
        ds = dstate[:, sl]
        dsb = ds.astype(BF)
        w = ex_w[:, sl]
        from_state = w * dot(bm, dsb)
        dxd = dot_tn(jnp.concatenate(mixb, axis=0), dstack) + from_state
        sums = sums + dot(
            jnp.concatenate(
                rbs + [(dy * carried).astype(BF), (xd * from_state).astype(BF), (x * dxd).astype(BF)], axis=1
            ),
            pick_ref[p],
        )
        f_sum = f_sum + dot(
            (ex_e[Q - 1 : Q, sl] * fold8(st * ds)), pick_ref[p, 2 * Q : 3 * Q, :].astype(F32)
        )
        edy = (e * dy).astype(BF)
        dC = dC + dot_nt(edy, stb)
        dB = dB + dot_nt((w * xd).astype(BF), dsb)
        dstate[:, sl] = ex_e[Q - 1 : Q, sl] * ds + dot(cm_t, edy)
        conv_back(sl, xdt * dxd + par_ref[6:7, sl] * dy, slope)
    dsc = dscores.astype(BF)
    conv_back(b_cols, dB + dot_tn(dsc, cm), b_slope)
    conv_back(c_cols, dC + dot(dsc, bm), c_slope)
    col_t = jnp.concatenate([cols, jnp.zeros((Q - 16, Q), F32)], axis=0).T
    row = lax.broadcasted_iota(jnp.int32, (Q, Q), 0)
    col = lax.broadcasted_iota(jnp.int32, (Q, Q), 1)
    lanes = lax.broadcasted_iota(jnp.int32, (Q, 128), 1)
    later = dot_hi((row <= col).astype(F32), sums - col_t)
    earlier = dot_hi((row > col).astype(F32), sums)
    da = later + pltpu.roll(earlier, 112, axis=1) + jnp.sum(f_sum, axis=0, keepdims=True)
    keep = lanes < n_heads
    ddt = da * rate + pltpu.roll(sums, 96, axis=1)
    draw = jnp.where(keep, ddt * jax.nn.sigmoid(raw), 0.0)
    gp_ref[:, 2 * width + 2 * NS :] = draw.astype(BF)
    acc[56:64, 0:128] += fold8(draw)
    acc[56:64, 128:256] += fold8(jnp.where(keep, da * dt * rate, 0.0))

    @pl.when(step == steps - 1)
    def _():
        rows = [jnp.sum(acc[8 * k : 8 * k + 8, :], axis=0, keepdims=True) for k in range(8)]
        acc_out[...] = jnp.concatenate(rows, axis=0)


def pick_table(width):
    pair = jnp.arange(width // 128)[:, None, None]
    row = jnp.arange(5 * Q)[None, :, None]
    lane = jnp.arange(128)[None, None, :]
    part, inner = row // Q, row % Q
    head = 2 * pair + jnp.where(part < 2, part, inner // 64)
    base = jnp.where(part == 3, 16, jnp.where(part == 4, 32, 0))
    return (lane == head + base).astype(BF)


def mixer_bwd(pre, par, pick, kept, dh, kap, width, n_heads):
    T = pre.shape[0]
    n = T // Q
    pw = pre.shape[1]
    wide = width + 2 * NS
    back = lambda cols: pl.BlockSpec((Q, cols), lambda i: (n - 1 - i, 0))
    return pl.pallas_call(
        functools.partial(bwd_kernel, width, n_heads),
        grid=(n,),
        in_specs=[
            back(pw),
            pl.BlockSpec(par.shape, lambda i: (0, 0)),
            pl.BlockSpec(pick.shape, lambda i: (0, 0, 0)),
            pl.BlockSpec((1, NS, width), lambda i: (n - 1 - i, 0, 0)),
            back(wide), back(width), back(width), back(width), back(width), back(128), back(128),
            back(width), back(128),
        ],
        out_specs=[back(pw), pl.BlockSpec((8, wide), lambda i: (0, 0))],
        out_shape=[jax.ShapeDtypeStruct((T, pw), BF), jax.ShapeDtypeStruct((8, wide), F32)],
        scratch_shapes=[pltpu.VMEM((Q + 8, wide), F32), pltpu.VMEM((NS, width), F32), pltpu.VMEM((64, wide), F32)],
        compiler_params=pltpu.CompilerParams(dimension_semantics=("arbitrary",), vmem_limit_bytes=56 << 20),
        cost_estimate=cost(35),
        name="mixer_bwd",
    )(pre, par, pick, *kept, dh, kap)


MESH_ID = pl.DeviceIdType.MESH


def peer(axis, index):
    return {axis: index}


def greet(peers):
    barrier = pltpu.get_barrier_semaphore()
    for where in peers:
        pl.semaphore_signal(barrier, inc=1, device_id=where, device_id_type=MESH_ID)
    pl.semaphore_wait(barrier, len(peers))


def remote(src, dst, send_sem, recv_sem, where):
    return pltpu.make_async_remote_copy(
        src_ref=src, dst_ref=dst, send_sem=send_sem, recv_sem=recv_sem,
        device_id=where, device_id_type=MESH_ID,
    )


PIECES = 2


def token_gather_kernel(count, *refs):
    ins, outs = refs[:count], refs[count : 2 * count]
    send_sem, recv_sem, own_sem = refs[2 * count :]
    me = lax.axis_index("tensor")
    near, far = me ^ 1, me ^ 2
    greet((peer("tensor", near), peer("tensor", far)))

    def copies(index):
        source, target = ins[index], outs[index]
        rows = source.shape[0]
        parts = PIECES if index == 0 else 1
        size = rows // parts
        for part in range(parts):
            here = pl.ds(part * size, size)
            own = pl.ds(pl.multiple_of(me * rows + part * size, 16), size)
            other = pl.ds(pl.multiple_of(far * rows + part * size, 16), size)
            to_far = remote(source.at[here], target.at[own], send_sem.at[index, part, 0],
                            recv_sem.at[index, part, 0], peer("tensor", far))
            to_near = remote(source.at[here], target.at[own], send_sem.at[index, part, 1],
                             recv_sem.at[index, part, 1], peer("tensor", near))
            relay = remote(target.at[other], target.at[other], send_sem.at[index, part, 2],
                           recv_sem.at[index, part, 2], peer("tensor", near))
            yield to_far, to_near, relay

    every = [triple for index in range(count) for triple in copies(index)]
    for to_far, _, _ in every:
        to_far.start()
    for _, to_near, _ in every:
        to_near.start()
    locals_ = []
    for index in range(count):
        rows = ins[index].shape[0]
        local_copy = pltpu.make_async_copy(
            ins[index], outs[index].at[pl.ds(pl.multiple_of(me * rows, 16), rows)], own_sem.at[index]
        )
        local_copy.start()
        locals_.append(local_copy)
    for to_far, _, relay in every:
        to_far.wait_recv()
        relay.start()
    for to_far, to_near, relay in every:
        to_near.wait_recv()
        relay.wait_recv()
        to_far.wait_send()
        to_near.wait_send()
        relay.wait_send()
    for local_copy in locals_:
        local_copy.wait()


def token_gather(values, group_id):
    count = len(values)
    n = lax.axis_size("tensor")
    return pl.pallas_call(
        functools.partial(token_gather_kernel, count),
        out_shape=[jax.ShapeDtypeStruct((n * v.shape[0],) + v.shape[1:], v.dtype) for v in values],
        in_specs=[pl.BlockSpec(memory_space=pltpu.VMEM)] * count,
        out_specs=[pl.BlockSpec(memory_space=pl.ANY)] * count,
        scratch_shapes=[
            pltpu.SemaphoreType.DMA((count, PIECES, 3)),
            pltpu.SemaphoreType.DMA((count, PIECES, 3)),
            pltpu.SemaphoreType.DMA((count,)),
        ],
        cost_estimate=cost(22),
        compiler_params=pltpu.CompilerParams(collective_id=group_id, has_side_effects=True),
        name="token_gather",
    )(*values)


RS_PIECES = 2


def token_scatter_kernel(with_side, *refs):
    if with_side:
        value_ref, side_ref, out_ref, side_out = refs[:4]
        rest = refs[4:]
    else:
        value_ref, out_ref = refs[:2]
        rest = refs[2:]
    from_near, to_far_buf, from_far, send_sem, recv_sem = rest[:5]
    me = lax.axis_index("tensor")
    near, far, cross = me ^ 1, me ^ 2, me ^ 3
    greet((peer("tensor", near), peer("tensor", far)))
    rows = out_ref.shape[0]
    size = rows // RS_PIECES

    def block(index, part):
        return pl.ds(pl.multiple_of(index * rows + part * size, 16), size)

    first, second, third = [], [], []
    for part in range(RS_PIECES):
        here = pl.ds(part * size, size)
        first.append(remote(value_ref.at[block(cross, part)], from_near.at[0, here], send_sem.at[part, 0],
                            recv_sem.at[part, 0], peer("tensor", near)))
        second.append(remote(value_ref.at[block(near, part)], from_near.at[1, here], send_sem.at[part, 1],
                             recv_sem.at[part, 1], peer("tensor", near)))
        third.append(remote(to_far_buf.at[here], from_far.at[here], send_sem.at[part, 2],
                            recv_sem.at[part, 2], peer("tensor", far)))
    for copy in first:
        copy.start()
    if with_side:
        side_near, side_buf, side_far, side_send, side_recv = rest[5:]
        srows = side_out.shape[0]

        def side_block(index):
            return pl.ds(pl.multiple_of(index * srows, 8), srows)

        s1 = remote(side_ref.at[side_block(cross)], side_near.at[0], side_send.at[0], side_recv.at[0], peer("tensor", near))
        s2 = remote(side_ref.at[side_block(near)], side_near.at[1], side_send.at[1], side_recv.at[1], peer("tensor", near))
        s3 = remote(side_buf, side_far, side_send.at[2], side_recv.at[2], peer("tensor", far))
        s1.start()
        s2.start()
    for copy in second:
        copy.start()
    if with_side:
        s1.wait_recv()
        side_buf[...] = side_ref[side_block(far), :] + side_near[0]
        s3.start()
    for part in range(RS_PIECES):
        here = pl.ds(part * size, size)
        first[part].wait_recv()
        to_far_buf[here, :] = (
            value_ref[block(far, part), :].astype(F32) + from_near[0, here, :].astype(F32)
        ).astype(to_far_buf.dtype)
        third[part].start()
    if with_side:
        s2.wait_recv()
        s3.wait_recv()
        side_out[...] = side_ref[side_block(me), :] + side_near[1] + side_far[...]
        s1.wait_send()
        s2.wait_send()
        s3.wait_send()
    for part in range(RS_PIECES):
        here = pl.ds(part * size, size)
        second[part].wait_recv()
        out_ref[here, :] = value_ref[block(me, part), :].astype(F32) + from_near[1, here, :].astype(F32)
    for part in range(RS_PIECES):
        here = pl.ds(part * size, size)
        third[part].wait_recv()
        out_ref[here, :] = out_ref[here, :] + from_far[here, :].astype(F32)
    for copy in first + second + third:
        copy.wait_send()


def token_scatter(value, group_id, side=None):
    n = lax.axis_size("tensor")
    rows, cols = value.shape[0] // n, value.shape[1]
    operands = [value]
    out_shape = [jax.ShapeDtypeStruct((rows, cols), F32)]
    scratch = [
        pltpu.VMEM((2, rows, cols), value.dtype),
        pltpu.VMEM((rows, cols), value.dtype),
        pltpu.VMEM((rows, cols), value.dtype),
        pltpu.SemaphoreType.DMA((RS_PIECES, 3)),
        pltpu.SemaphoreType.DMA((RS_PIECES, 3)),
    ]
    if side is not None:
        srows, scols = side.shape[0] // n, side.shape[1]
        operands.append(side)
        out_shape.append(jax.ShapeDtypeStruct((srows, scols), F32))
        scratch += [
            pltpu.VMEM((2, srows, scols), F32),
            pltpu.VMEM((srows, scols), F32),
            pltpu.VMEM((srows, scols), F32),
            pltpu.SemaphoreType.DMA((3,)),
            pltpu.SemaphoreType.DMA((3,)),
        ]
    return pl.pallas_call(
        functools.partial(token_scatter_kernel, side is not None),
        out_shape=out_shape,
        in_specs=[pl.BlockSpec(memory_space=pltpu.VMEM)] * len(operands),
        out_specs=[pl.BlockSpec(memory_space=pltpu.VMEM)] * len(operands),
        scratch_shapes=scratch,
        cost_estimate=cost(22),
        compiler_params=pltpu.CompilerParams(collective_id=group_id, has_side_effects=True, vmem_limit_bytes=40 << 20),
        name="token_scatter",
    )(*operands)


def open_kernel(n, pieces, tokens, *refs):
    if tokens:
        in_ref, xn_ref, fin_ref, xall_ref, x_ss, x_rs, z_ss, z_rs, own_sem, t_ss, t_rs = refs
    else:
        in_ref, fin_ref, x_ss, x_rs, z_ss, z_rs, own_sem = refs
    sec, z, ten = lax.axis_index("section"), lax.axis_index("dp"), lax.axis_index("tensor")
    across = peer("section", 1 - sec)
    near, far = peer("tensor", ten ^ 1), peer("tensor", ten ^ 2)
    barrier = pltpu.get_barrier_semaphore()
    for where in (across, near, far) if tokens else (across,):
        pl.semaphore_signal(barrier, inc=1, device_id=where, device_id_type=MESH_ID)

    @pl.when(z > 0)
    def _():
        pl.semaphore_signal(barrier, inc=1, device_id=peer("dp", z - 1), device_id_type=MESH_ID)

    @pl.when(z < n - 1)
    def _():
        pl.semaphore_signal(barrier, inc=1, device_id=peer("dp", z + 1), device_id_type=MESH_ID)

    pl.semaphore_wait(barrier, (3 if tokens else 1) + jnp.where(z > 0, 1, 0) + jnp.where(z < n - 1, 1, 0))
    sources, fulls = (in_ref,), (fin_ref,)
    rows = in_ref.shape[0]

    def place(p, s):
        array, offset, count, _ = pieces[p]
        return fulls[array].at[pl.ds(pl.multiple_of(s * rows + offset, 16), count)]

    def own(p):
        array, offset, count, _ = pieces[p]
        return sources[array].at[pl.ds(offset, count)]

    def to_x(p, s, source):
        return remote(source, place(p, s), x_ss.at[p, s], x_rs.at[p, s], across)

    def to_z(p, s, step, source):
        side = 0 if step > 0 else 1
        return remote(source, place(p, s), z_ss.at[side, p, s], z_rs.at[side, p, s], peer("dp", z + step))

    def got_z(p, s, side):
        remote(own(p), place(p, s), z_ss.at[side, p, 0], z_rs.at[side, p, s], across).wait_recv()

    def spread(p, s, source, right=True, left=True):
        if right:
            @pl.when(z < n - 1)
            def _():
                to_z(p, s, 1, source).start()
        if left:
            @pl.when(z > 0)
            def _():
                to_z(p, s, -1, source).start()

    every = range(len(pieces))
    via = [piece[3] for piece in pieces]
    if tokens:
        trows = xn_ref.shape[0]
        me = pl.ds(pl.multiple_of(ten * trows, 16), trows)
        other = pl.ds(pl.multiple_of((ten ^ 2) * trows, 16), trows)
        tok_far = remote(xn_ref, xall_ref.at[me], t_ss.at[0], t_rs.at[0], far)
        tok_near = remote(xn_ref, xall_ref.at[me], t_ss.at[1], t_rs.at[1], near)
        tok_relay = remote(xall_ref.at[other], xall_ref.at[other], t_ss.at[2], t_rs.at[2], near)
        tok_own = pltpu.make_async_copy(xn_ref, xall_ref.at[me], own_sem.at[0])
        tok_far.start()
        tok_near.start()
        tok_own.start()

    @pl.when(sec == 0)
    def _():
        for p in every:
            if via[p] == 1:
                to_x(p, z, own(p)).start()
            else:
                spread(p, z, own(p))
        for p in every:
            if via[p] == 0:
                to_x(p, z, own(p)).start()
        for array in (0,):
            whole = fulls[array].at[pl.ds(pl.multiple_of(z * rows, 16), rows)]
            pltpu.make_async_copy(sources[array], whole, own_sem.at[1 + array]).start()
        for d in range(1, n):
            for p in every:
                if via[p] == 0:
                    @pl.when(z - d >= 0)
                    def _():
                        got_z(p, z - d, 0)
                        spread(p, z - d, place(p, z - d), left=False)
                        to_x(p, z - d, place(p, z - d)).start()

                    @pl.when(z + d < n)
                    def _():
                        got_z(p, z + d, 1)
                        spread(p, z + d, place(p, z + d), right=False)
                        to_x(p, z + d, place(p, z + d)).start()
        for d in range(1, n):
            s = lax.rem(z + d, n)
            for p in every:
                if via[p] == 1:
                    to_x(p, s, place(p, s)).wait_recv()

    @pl.when(sec == 1)
    def _():
        for p in every:
            if via[p] == 1:
                to_x(p, z, place(p, z)).wait_recv()
                spread(p, z, place(p, z))
        for d in range(1, n):
            for p in every:
                if via[p] == 1:
                    @pl.when(z - d >= 0)
                    def _():
                        got_z(p, z - d, 0)
                        spread(p, z - d, place(p, z - d), left=False)
                        to_x(p, z - d, place(p, z - d)).start()

                    @pl.when(z + d < n)
                    def _():
                        got_z(p, z + d, 1)
                        spread(p, z + d, place(p, z + d), right=False)
                        to_x(p, z + d, place(p, z + d)).start()
        for d in range(n):
            s = lax.rem(z + d, n)
            for p in every:
                if via[p] == 0:
                    to_x(p, s, place(p, s)).wait_recv()

    if tokens:
        tok_far.wait_recv()
        tok_relay.start()
        tok_near.wait_recv()
        tok_relay.wait_recv()
        for copy in (tok_far, tok_near, tok_relay):
            copy.wait_send()
        tok_own.wait()

    @pl.when(sec == 0)
    def _():
        for array in (0,):
            whole = fulls[array].at[pl.ds(pl.multiple_of(z * rows, 16), rows)]
            pltpu.make_async_copy(sources[array], whole, own_sem.at[1 + array]).wait()

    for p in every:
        for d in range(n):
            s = lax.rem(z + d, n)
            mine = sec == via[p]
            if d == 0:
                sent_x = jnp.logical_or(sec == 0, False)
            else:
                sent_x = mine

            @pl.when(sent_x)
            def _():
                to_x(p, s, place(p, s)).wait_send()

            @pl.when(mine & (s <= z) & (z < n - 1))
            def _():
                to_z(p, s, 1, place(p, s)).wait_send()

            @pl.when(mine & (s >= z) & (z > 0))
            def _():
                to_z(p, s, -1, place(p, s)).wait_send()


def open_gather(own, group_id, xn=None):
    n = lax.axis_size("dp")
    rows = own.shape[0]
    first = max(1, round(rows * 5 / 12 / 16)) * 16
    rest = (rows - first) // 2
    pieces = ((0, first, rest, 1), (0, first + rest, rest, 1), (0, 0, first, 0))
    count = len(pieces)
    sem = lambda *shape: pltpu.SemaphoreType.DMA(shape)
    operands, out_shape = [own], [jax.ShapeDtypeStruct((n * rows, own.shape[1]), BF)]
    scratch = [sem(count, n), sem(count, n), sem(2, count, n), sem(2, count, n), sem(3)]
    if xn is not None:
        operands.append(xn)
        out_shape.append(jax.ShapeDtypeStruct((lax.axis_size("tensor") * xn.shape[0], xn.shape[1]), BF))
        scratch += [sem(3), sem(3)]
    return pl.pallas_call(
        functools.partial(open_kernel, n, pieces, xn is not None),
        out_shape=out_shape,
        in_specs=[pl.BlockSpec(memory_space=pltpu.VMEM)] * len(operands),
        out_specs=[pl.BlockSpec(memory_space=pl.ANY)] * len(operands),
        scratch_shapes=scratch,
        cost_estimate=cost(90 if xn is not None else 40),
        compiler_params=pltpu.CompilerParams(collective_id=group_id, has_side_effects=True),
        name="weights_open",
    )(*operands)


CHUNK_ROWS = 16


def by_rows(count, body):
    @pl.loop(0, count // CHUNK_ROWS)
    def _(index):
        body(pl.multiple_of(index * CHUNK_ROWS, CHUNK_ROWS))


def finish_kernel(
    n, bc_at, gain_rows,
    g_ref, mid_ref, half_ref, own_ref, gp_ref, w_ref, u_ref, seed_ref, inv_ref, gain_ref, small_ref,
    gin_ref, gout_ref, small_x_ref, small_t_ref, bc_ref, du_ref, du_got_ref,
    x_recv, z_recv, z_send, o_recv, o_send, last_buf, last_recv, join_recv, olast_buf, olast_recv,
    part_a, part_b, near_recv, far_send, far_recv, dxn, gain_acc,
    small_own, small_recv, small_all, small_ten, bc_own, bc_far, bc_mid, bc_near,
    x_ss, x_rs, z_ss, z_rs, o_ss, o_rs, m_ss, m_rs, d_ss, d_rs, t_ss, t_rs, y_ss, y_rs,
):
    sec, z, ten = lax.axis_index("section"), lax.axis_index("dp"), lax.axis_index("tensor")
    half, wide = half_ref.shape
    rows = 2 * half
    mine, theirs = sec * half, (1 - sec) * half
    across = peer("section", 1 - sec)
    near, far = peer("tensor", ten ^ 1), peer("tensor", ten ^ 2)
    others = [lax.rem(z + d, n) for d in range(1, n)]
    mates = [ten ^ d for d in range(1, 4)]
    greet([across] + [peer("dp", o) for o in others] + [peer("tensor", t) for t in mates])
    cut = wide // 256 * 128
    columns = (slice(cut, wide), slice(0, cut))
    order = [i // 2 if i % 2 else n - 1 - i // 2 for i in range(n)]

    def shard_rows(s, offset):
        return pl.ds(pl.multiple_of(s * rows + offset, 16), half)

    x_copies = {}
    for c, cols in enumerate(columns):
        for s in order:
            x_copies[c, s] = remote(
                g_ref.at[shard_rows(s, theirs), cols], x_recv.at[s, :, cols], x_ss.at[c, s], x_rs.at[c, s], across
            )
    early = [(0, s) for s in order] + [(1, order[0])]
    for key in early:
        x_copies[key].start()
    join = remote(half_ref, join_recv, m_ss.at[0], m_rs.at[0], across)
    ojoin = remote(own_ref, olast_recv, m_ss.at[1], m_rs.at[1], across)
    olast = remote(olast_buf, olast_recv, m_ss.at[1], m_rs.at[1], across)
    lasts = [
        remote(last_buf.at[:, cols], last_recv.at[:, cols], m_ss.at[2 + c], m_rs.at[2 + c], across)
        for c, cols in enumerate(columns)
    ]
    du_copy = remote(du_ref, du_got_ref, m_ss.at[4], m_rs.at[4], across)

    @pl.when(sec == 0)
    def _():
        ojoin.start()

    trows = u_ref.shape[0]
    step = 256
    tiles = w_ref.shape[0] // step

    def product(index, put):
        @pl.loop(0, tiles)
        def _(tile):
            at = pl.ds(pl.multiple_of(tile * step, step), step)
            put(at, dot_nt(gp_ref[pl.ds(pl.multiple_of(index * trows, 16), trows), :], w_ref[at, :]))

    y_cross = remote(part_a, near_recv.at[0], y_ss.at[0], y_rs.at[0], near)
    y_near = remote(part_b, near_recv.at[1], y_ss.at[1], y_rs.at[1], near)
    y_far = remote(far_send, far_recv, y_ss.at[2], y_rs.at[2], far)

    def put_a(at, value):
        part_a[:, at] = value.astype(BF)

    def put_b(at, value):
        part_b[:, at] = value.astype(BF)

    def put_far(at, value):
        far_send[:, at] = (value + near_recv[0, :, at].astype(F32)).astype(BF)

    def put_own(at, value):
        dxn[:, at] = value

    product(ten ^ 3, put_a)
    y_cross.start()
    product(ten ^ 1, put_b)
    y_near.start()
    y_cross.wait_recv()
    product(ten ^ 2, put_far)
    y_far.start()
    product(ten, put_own)

    def down(s):
        right = s > z
        return jnp.where(right, 0, 1), peer("dp", z + jnp.where(right, 1, -1)), jnp.where(right, z > 0, z < n - 1)

    def reduce_step(s, plain, recv, send, ss, rs, cols):
        @pl.when(s != z)
        def _():
            side, below, upstream = down(s)

            @pl.when(upstream)
            def _():
                remote(send.at[s, :, cols], recv.at[side, s, :, cols], ss.at[s], rs.at[side, s], across).wait_recv()

                def body(r):
                    at = pl.ds(r, CHUNK_ROWS)
                    send[s, at, cols] = (plain(s, r, cols) + recv[side, s, at, cols].astype(F32)).astype(BF)

                by_rows(half, body)

            @pl.when(jnp.logical_not(upstream))
            def _():
                def body(r):
                    send[s, pl.ds(r, CHUNK_ROWS), cols] = plain(s, r, cols).astype(BF)

                by_rows(half, body)

            remote(send.at[s, :, cols], recv.at[side, s, :, cols], ss.at[s], rs.at[side, s], below).start()

    def reduce_own(plain, recv, ss, rs, send, cols, target):
        def base(r):
            target[pl.ds(r, CHUNK_ROWS), cols] = plain(z, r, cols)

        by_rows(half, base)
        for side, there in ((0, z > 0), (1, z < n - 1)):

            @pl.when(there)
            def _():
                remote(send.at[0, :, cols], recv.at[side, z, :, cols], ss.at[0], rs.at[side, z], across).wait_recv()

                def more(r):
                    at = pl.ds(r, CHUNK_ROWS)
                    target[at, cols] += recv[side, z, at, cols].astype(F32)

                by_rows(half, more)

    def reduce_done(send, recv, ss, rs, cols):
        for s in order:
            @pl.when(s != z)
            def _():
                side, below, _ = down(s)
                remote(send.at[s, :, cols], recv.at[side, s, :, cols], ss.at[s], rs.at[side, s], below).wait_send()

    def in_plain(s, r, cols):
        at = pl.ds(pl.multiple_of(s * rows + mine + r, 16), CHUNK_ROWS)
        return g_ref[at, cols].astype(F32) + x_recv[s, pl.ds(r, CHUNK_ROWS), cols].astype(F32)

    def out_plain(s, r, cols):
        return mid_ref[pl.ds(pl.multiple_of(s * half + r, 16), CHUNK_ROWS), cols].astype(F32)

    ocols = slice(0, own_ref.shape[1])

    def in_step(c, k):
        s = order[k]
        x_copies[c, s].wait_recv()
        reduce_step(s, in_plain, x_in, z_in, z_ss.at[c], z_rs.at[c], columns[c])

    x_in, z_in = z_recv, z_send
    for s in order:
        reduce_step(s, out_plain, o_recv, o_send, o_ss, o_rs, ocols)
    in_step(0, 0)
    in_step(0, 1)
    y_near.wait_recv()
    y_far.wait_recv()
    gain_acc[...] = jnp.zeros_like(gain_acc)
    model = u_ref.shape[1]

    def du_rows(r):
        at = pl.ds(r, CHUNK_ROWS)
        u = u_ref[at, :].astype(F32)
        inv = inv_ref[at, :]
        grad = dxn[at, :] + near_recv[1, at, :].astype(F32) + far_recv[at, :].astype(F32)
        scaled = grad * gain_ref[...]
        dots = jnp.sum(scaled * u, axis=1, keepdims=True)
        du_ref[at, :] = (seed_ref[at, :].astype(F32) + inv * scaled - u * (inv * inv * inv * dots / model)).astype(BF)
        gain_acc[...] += fold8(grad * u * inv)

    by_rows(trows, du_rows)

    srows, swide = small_recv.shape
    small_own[...] = small_ref[...]
    gain_sum = jnp.sum(gain_acc[...], axis=0, keepdims=True)
    for k in range(gain_rows):
        part = gain_sum[:, k * swide : min((k + 1) * swide, model)]
        small_own[8 + k : 9 + k, 0 : part.shape[1]] = part
    small_x = remote(small_own.at[pl.ds(pl.multiple_of((1 - sec) * srows, 8), srows)], small_recv,
                     m_ss.at[5], m_rs.at[5], across)
    small_x.start()
    for key, copy in x_copies.items():
        if key not in early:
            copy.start()

    @pl.when(sec == 1)
    def _():
        du_copy.start()

    @pl.when(sec == 0)
    def _():
        join.start()

    for k in range(2, n):
        in_step(0, k)
    small_x.wait_recv()
    small_all[z] = small_own[pl.ds(pl.multiple_of(sec * srows, 8), srows), :] + small_recv[...]
    to_dp = [remote(small_all.at[z], small_all.at[z], d_ss.at[d], d_rs.at[z], peer("dp", o)) for d, o in enumerate(others)]
    for copy in to_dp:
        copy.start()
    reduce_own(out_plain, o_recv, o_ss, o_rs, o_send, ocols, gout_ref)

    def halves(own_part, got, target, cols, own_first):
        def put(r):
            at, low = pl.ds(r, CHUNK_ROWS), pl.ds(pl.multiple_of(half + r, 16), CHUNK_ROWS)
            if own_first:
                target[low, cols] = got[at, cols].astype(F32)
            else:
                target[at, cols] = got[at, cols].astype(F32)
                target[low, cols] = own_part[at, cols].astype(F32)

        by_rows(half, put)

    def hand_over(target, buffer, cols):
        def put(r):
            at = pl.ds(r, CHUNK_ROWS)
            buffer[at, cols] = target[at, cols].astype(BF)

        by_rows(half, put)

    @pl.when(sec == 1)
    def _():
        hand_over(gout_ref, olast_buf, ocols)
        olast.start()

    def start_bc():
        bc_own[...] = gin_ref[:, bc_at : bc_at + 2 * NS].astype(BF)
        remote(bc_own, bc_far, t_ss.at[3], t_rs.at[4], far).start()

    for c, cols in enumerate(columns):
        if c:
            for k in range(n):
                in_step(c, k)
            for d, o in enumerate(others):
                remote(small_all.at[o], small_all.at[o], d_ss.at[d], d_rs.at[o], across).wait_recv()
            total = small_all[0]
            for k in range(1, n):
                total = total + small_all[k]
            small_x_ref[...] = total
            small_ten[ten] = total
            to_ten = [
                remote(small_ten.at[ten], small_ten.at[ten], t_ss.at[d], t_rs.at[ten], peer("tensor", t))
                for d, t in enumerate(mates)
            ]
            for copy in to_ten:
                copy.start()
        reduce_own(in_plain, x_in, z_ss.at[c], z_rs.at[c], z_in, cols, gin_ref)

        @pl.when(sec == 1)
        def _():
            hand_over(gin_ref, last_buf, cols)
            lasts[c].start()

    @pl.when(sec == 1)
    def _():
        olast.wait_recv()
        halves(own_ref, olast_recv, gout_ref, ocols, False)
        join.wait_recv()
        for cols in columns:
            halves(half_ref, join_recv, gin_ref, cols, False)
        start_bc()

    @pl.when(sec == 0)
    def _():
        lasts[0].wait_recv()
        halves(None, last_recv, gin_ref, columns[0], True)
        start_bc()
        olast.wait_recv()
        halves(None, olast_recv, gout_ref, ocols, True)
        lasts[1].wait_recv()
        halves(None, last_recv, gin_ref, columns[1], True)
        du_copy.wait_recv()
        ojoin.wait_send()
        join.wait_send()

    for d, t in enumerate(mates):
        remote(small_ten.at[t], small_ten.at[t], t_ss.at[d], t_rs.at[t], near).wait_recv()
    total = small_ten[0]
    for k in range(1, 4):
        total = total + small_ten[k]
    small_t_ref[...] = total
    to_far = remote(bc_own, bc_far, t_ss.at[3], t_rs.at[4], far)
    to_far.wait_recv()
    bc_mid[...] = (bc_own[...].astype(F32) + bc_far[...].astype(F32)).astype(BF)
    to_near = remote(bc_mid, bc_near, t_ss.at[4], t_rs.at[5], near)
    to_near.start()
    to_near.wait_recv()
    bc_ref[...] = bc_mid[...].astype(F32) + bc_near[...].astype(F32)
    for c, cols in enumerate(columns):
        for s in order:
            x_copies[c, s].wait_send()
        reduce_done(z_in, x_in, z_ss.at[c], z_rs.at[c], cols)
    reduce_done(o_send, o_recv, o_ss, o_rs, ocols)

    @pl.when(sec == 1)
    def _():
        olast.wait_send()
        for copy in lasts:
            copy.wait_send()
        du_copy.wait_send()

    for copy in [small_x, to_far, to_near, y_cross, y_near, y_far] + to_dp + to_ten:
        copy.wait_send()


def finish(grads, out_mid, half_other, out_other, gp, w_in, u, seed, inv, gain, smalls, bc_at, gain_rows, group_id):
    n = lax.axis_size("dp")
    half, wide = half_other.shape
    owide = out_other.shape[1]
    trows, model = u.shape
    srows, swide = smalls.shape[0] // 2, smalls.shape[1]
    vm = lambda dtype, *shape: pltpu.VMEM(shape, dtype)
    sem = lambda *shape: pltpu.SemaphoreType.DMA(shape)
    return pl.pallas_call(
        functools.partial(finish_kernel, n, bc_at, gain_rows),
        out_shape=[
            jax.ShapeDtypeStruct((2 * half, wide), F32),
            jax.ShapeDtypeStruct((2 * half, owide), F32),
            jax.ShapeDtypeStruct((srows, swide), F32),
            jax.ShapeDtypeStruct((srows, swide), F32),
            jax.ShapeDtypeStruct((2 * half, 2 * NS), F32),
            jax.ShapeDtypeStruct((trows, model), BF),
            jax.ShapeDtypeStruct((trows, model), BF),
        ],
        in_specs=[pl.BlockSpec(memory_space=pltpu.VMEM)] * 11,
        out_specs=[pl.BlockSpec(memory_space=pltpu.VMEM)] * 7,
        scratch_shapes=[
            vm(BF, n, half, wide), vm(BF, 2, n, half, wide), vm(BF, n, half, wide),
            vm(BF, 2, n, half, owide), vm(BF, n, half, owide),
            vm(BF, half, wide), vm(BF, half, wide), vm(BF, half, wide), vm(BF, half, owide), vm(BF, half, owide),
            vm(BF, trows, model), vm(BF, trows, model), vm(BF, 2, trows, model), vm(BF, trows, model),
            vm(BF, trows, model), vm(F32, trows, model), vm(F32, 8, model),
            vm(F32, 2 * srows, swide), vm(F32, srows, swide), vm(F32, n, srows, swide), vm(F32, 4, srows, swide),
            vm(BF, 2 * half, 2 * NS), vm(BF, 2 * half, 2 * NS), vm(BF, 2 * half, 2 * NS), vm(BF, 2 * half, 2 * NS),
            sem(2, n), sem(2, n), sem(2, n), sem(2, 2, n), sem(n), sem(2, n),
            sem(6), sem(6), sem(n), sem(n), sem(5), sem(6), sem(3), sem(3),
        ],
        cost_estimate=cost(120),
        compiler_params=pltpu.CompilerParams(collective_id=group_id, has_side_effects=True, vmem_limit_bytes=63 << 20),
        name="grad_finish",
    )(grads, out_mid, half_other, out_other, gp, w_in, u, seed, inv, gain, smalls)


EPSILON = 1e-05
HEAD_PAD = 128
SMALL_ROWS = 16


def swap_sections(value):
    count = lax.axis_size("section")
    return lax.ppermute(value, "section", [(i, (i + 1) % count) for i in range(count)])


def later_gather(own, is_first, after):
    half = own.shape[0] // 2
    low, high = own[:half], own[half:]
    got = lax.ppermute(low, "section", [(1, 0)])
    piece, after = lax.optimization_barrier((jnp.where(is_first, got, high), after))
    return lax.all_gather(piece, ("dp", "section"), axis=0, tiled=True), after


def grad_scatter(value):
    return lax.psum_scatter(value, ("dp", "section"), scatter_dimension=0, tiled=True)


def local(
    stream, cotangent, norm_gain, in_zx, in_dt, in_bc, out_proj, conv_x, conv_x_bias,
    conv_bc, conv_bc_bias, dt_bias, a_log, d_skip, gate_gain,
):
    section = lax.axis_index("section")
    is_first = section == 0
    model = stream.shape[3]
    rows = stream.shape[2]
    width = conv_x.shape[2]
    heads = dt_bias.shape[1]
    shard = in_zx.shape[1]
    total_inner = width * lax.axis_size("tensor")
    wide = width + 2 * NS

    def padded(value):
        return jnp.pad(value, (0, wide - value.shape[0]))[None]

    gain_rows = -(-model // wide)
    own_par = jnp.concatenate(
        [
            jnp.concatenate([conv_x[0], conv_bc[0]], axis=1),
            jnp.concatenate([conv_x_bias[0], conv_bc_bias[0]])[None],
            padded(gate_gain[0]),
            padded(jnp.repeat(d_skip[0], width // heads)),
            padded(dt_bias[0]),
            padded(a_log[0]),
            jnp.pad(norm_gain[0], (0, gain_rows * wide - model)).reshape(gain_rows, wide),
            jnp.zeros((7 - gain_rows, wide), F32),
        ],
        axis=0,
    )
    other_par = swap_sections(own_par)
    pars = (jnp.where(is_first, own_par, other_par), jnp.where(is_first, other_par, own_par))
    gains = tuple(par[9 : 9 + gain_rows].reshape(-1)[:model] for par in pars)

    own_in = jnp.concatenate(
        [
            in_zx[0].reshape(shard, 2 * width),
            in_bc[0],
            jnp.pad(in_dt[0], ((0, 0), (0, HEAD_PAD - heads))),
        ],
        axis=1,
    )
    own_out = out_proj[0].T

    head_of = jnp.arange(width) // (width // heads)
    spread = (jnp.arange(2 * HEAD_PAD)[:, None] % HEAD_PAD == head_of[None, :]).astype(BF)
    pick = pick_table(width)

    def normed(layer, u):
        inv = lax.rsqrt(jnp.mean(u * u, axis=1, keepdims=True) + EPSILON)
        return inv, (u * inv * gains[layer][None, :]).astype(BF)

    def forward(layer, u, inv, xn, w_in, w_out):
        pre = dot(xn, w_in)
        yn, squares, *saved = mixer_fwd(pre, pars[layer], spread, width)
        partial = dot_nt(yn, w_out).astype(BF)
        total, squares = token_scatter(partial, 3 + layer, squares)
        q = lax.rsqrt(squares[::8].reshape(rows) / total_inner + EPSILON)[:, None]
        projected = total * q
        return (u + projected).astype(BF), (u, inv, xn, pre, yn, saved, q, projected, w_in, w_out)

    def backward_core(layer, g, kept):
        u, inv, xn, pre, yn, saved, q, projected, w_in, w_out = kept
        kappa = q * q / total_inner * jnp.sum(g * projected, axis=1, keepdims=True)
        high = kappa.astype(BF)
        low = (kappa - high.astype(F32)).astype(BF)
        side = jnp.pad(jnp.concatenate([high, low], axis=1), ((0, 0), (0, 126)))
        gq, side = token_gather([(g * q).astype(BF), side], 5 + layer)
        g_out = dot_tn(gq, yn).astype(BF)
        dh = dot(gq, w_out)
        gp, acc = mixer_bwd(pre, pars[layer], pick, saved, dh, side, width, heads)
        g_in = dot_tn(xn, gp).astype(BF)
        return gp, acc, g_in, g_out

    def backward_input(layer, g, kept, gp):
        u, inv = kept[:2]
        (dxn,) = token_scatter(dot_nt(gp, kept[8]).astype(BF), 7 + layer)
        scaled = dxn * gains[layer][None, :]
        dots = jnp.sum(scaled * u, axis=1, keepdims=True)
        du = g + inv * scaled - u * (inv * inv * inv) * dots / model
        return du.astype(BF), jnp.sum(dxn * u * inv, axis=0)

    def cross_sum(value):
        split = value.reshape(-1, 2, shard // 2, width)
        mine = jnp.where(is_first, split[:, 0], split[:, 1])
        theirs = swap_sections(jnp.where(is_first, split[:, 1], split[:, 0]))
        return (mine.astype(F32) + theirs.astype(F32)).astype(BF).reshape(-1, width)

    stream_own = lax.dynamic_index_in_dim(stream[:, 0], section, 0, False)
    u0 = stream_own.astype(F32)
    inv0, xn0 = normed(0, u0)
    w_in0, xn0 = open_gather(own_in, 1, xn0)
    full_in1, w_in0 = later_gather(own_in, is_first, w_in0)
    own_out0, w_in0 = lax.optimization_barrier((own_out, w_in0))
    (w_out0,) = open_gather(own_out0, 10)
    full_out1, w_out0 = later_gather(own_out, is_first, w_out0)

    out0, kept0 = forward(0, u0, inv0, xn0, w_in0, w_out0)
    u1 = out0.astype(F32)
    inv1, xn1 = normed(1, u1)
    (xn1,) = token_gather([xn1], 2)
    out1, kept1 = forward(1, u1, inv1, xn1, full_in1, full_out1)
    g1 = lax.dynamic_index_in_dim(cotangent[:, 0], section, 0, False).astype(F32)
    gp1, acc1, g_in1, g_out1 = backward_core(1, g1, kept1)
    half_out1 = lax.psum_scatter(cross_sum(g_out1), "dp", scatter_dimension=0, tiled=True)
    half_in1 = grad_scatter(g_in1)
    gp1, g_in1 = lax.optimization_barrier((gp1, g_in1))
    du1, gain1 = backward_input(1, g1, kept1, gp1)
    gp0, acc0, g_in0, g_out0 = backward_core(0, du1.astype(F32), kept0)
    out_mid = cross_sum(g_out0)
    du1_first = lax.ppermute(du1, "section", [(0, 1)])

    def by_batch(first_value, second_value):
        own = jnp.where(is_first, first_value, second_value)
        got = swap_sections(jnp.where(is_first, second_value, first_value))
        stacked = jnp.stack([jnp.where(is_first, own, got), jnp.where(is_first, got, own)])
        return stacked[None, :, None]

    def minor(acc, gain):
        return jnp.concatenate(
            [
                acc,
                jnp.pad(gain, (0, gain_rows * wide - model)).reshape(gain_rows, wide),
                jnp.zeros((SMALL_ROWS - 8 - gain_rows, wide), F32),
            ],
            axis=0,
        )

    smalls = jnp.concatenate([minor(acc0, jnp.zeros_like(gain1)), minor(acc1, gain1)])
    g_in, g_out, mine, shared, bc_rows, du0, du0_second = finish(
        g_in0, out_mid, half_in1, half_out1, gp0, w_in0, stream_own, du1, inv0, gains[0][None, :],
        smalls, 2 * width, gain_rows, 9,
    )
    grads = jnp.stack([jnp.where(is_first, du0, du1_first), jnp.where(is_first, du0_second, du1)])
    return (
        by_batch(out0, out1),
        grads[None, :, None],
        shared[8 : 8 + gain_rows].reshape(-1)[:model][None],
        g_in[:, : 2 * width].reshape(shard, 2, width)[None],
        g_in[:, 2 * width + 2 * NS : 2 * width + 2 * NS + heads][None],
        bc_rows[None],
        g_out.T[None],
        mine[0:4, :width][None],
        mine[4, :width][None],
        shared[0:4, width:][None],
        shared[4, width:][None],
        mine[7, :heads][None],
        mine[7, HEAD_PAD : HEAD_PAD + heads][None],
        mine[6, :width].reshape(heads, -1).sum(axis=1)[None],
        mine[5, :width][None],
    )


def solution(mesh):
    in_specs = (
        P(None, "dp", "tensor", None),
        P(None, "dp", "tensor", None),
        P("section", None),
        P("section", "dp", None, "tensor"),
        P("section", "dp", "tensor"),
        P("section", "dp", None),
        P("section", "tensor", "dp"),
        P("section", None, "tensor"),
        P("section", "tensor"),
        P("section", None, None),
        P("section", None),
        P("section", "tensor"),
        P("section", "tensor"),
        P("section", "tensor"),
        P("section", "tensor"),
    )
    out_specs = (
        P("section", None, "dp", "tensor", None),
        P("section", None, "dp", "tensor", None),
        P("section", None),
        P("section", "dp", None, "tensor"),
        P("section", "dp", "tensor"),
        P("section", "dp", None),
        P("section", "tensor", "dp"),
        P("section", None, "tensor"),
        P("section", "tensor"),
        P("section", None, None),
        P("section", None),
        P("section", "tensor"),
        P("section", "tensor"),
        P("section", "tensor"),
        P("section", "tensor"),
    )
    return jax.shard_map(local, mesh=mesh, in_specs=in_specs, out_specs=out_specs, check_vma=False)
```
